512 devices in a mesh: local: 4 (over y), dp: 128 (over z, x, core).
Axes of the slice: x: 4, y: 4, z: 16, core: 2. Of those that a mesh axis runs over, the one named last changes fastest.
Arguments:
- gradient: bfloat16 [512, 72, 7168], P(('local', 'dp')), may hold values from -1.1953125 to 1.1953125
- feedback: bfloat16 [512, 72, 7168], P(('local', 'dp')), may hold values from -0.59765625 to 0.59765625
- basis_in: float32 [7168, 32], replicated, may hold values from -6 to 6
Outputs:
- new_feedback: bfloat16 [512, 72, 7168], P(('local', 'dp'))
- new_basis: float32 [7168, 32], replicated
The draws below stay inside these ranges and needn't reach their ends.
All inputs are finite; a program needn't handle non-finite values.
Results may differ from the reference program's by a relative error of at most 0.001.
Values sent between devices are 32-bit elements; how exact they have to be, the bound alone decides.
A program may use at most 64 MiB of HBM per device.

```python
import jax
import jax.numpy as jnp
from jax import lax

ROWS = 72
FF = 7168
RANK = 32
WORKERS = 512


def level_of(rng, dims, split, least, largest):
    gain = 1.0
    for position, shards_of in split:
        draws = jax.random.uniform(jax.random.fold_in(jax.random.fold_in(rng, 6), position), (shards_of,), jnp.float32, least / len(split), largest / len(split))
        gain = gain * jnp.repeat(jnp.exp(draws), dims[position] // shards_of).reshape((-1,) + (1,) * (len(dims) - 1 - position))
    return gain


def gaussian(own_key, extent, scale, limit, cuts=(), kind=jnp.bfloat16):
    factor_of = level_of(own_key, extent, cuts, -0.22, 0.18) if cuts else 1.0
    array = jax.random.normal(own_key, extent, jnp.float32) * scale * factor_of
    return jnp.minimum(jnp.maximum(array, -limit), limit).astype(kind)


def setup_inputs(seed: int = 0) -> dict:
    arg_keys = jax.random.split(jax.random.key(seed), 4)
    return {
        "gradient": gaussian(arg_keys[0], (WORKERS, ROWS, FF), 0.2, 1.1953125, ((0, 512),)),
        "feedback": gaussian(arg_keys[1], (WORKERS, ROWS, FF), 0.1, 0.59765625, ((0, 512),)),
        "basis_in": gaussian(arg_keys[2], (FF, RANK), 1.0, 6.0, (), jnp.float32),
    }


epsilon = 1e-06

def orthonormal(matrix):
    columns = []
    for column in range(matrix.shape[1]):
        vector = matrix[:, column]
        for earlier in columns:
            vector = vector - jnp.sum(earlier * vector) * earlier
        vector = vector * lax.rsqrt(jnp.sum(vector * vector) + epsilon)
        columns.append(vector)
    return jnp.stack(columns, axis=1)

def reference(gradient, feedback, basis_in):
    highest = lax.Precision.HIGHEST
    indices = jnp.arange(WORKERS, dtype=jnp.int32)

    def merged_of(index):
        return gradient[index].astype(jnp.float32) + feedback[index].astype(jnp.float32)

    def add_left(carry, index):
        return (carry + jnp.dot(merged_of(index), basis_in, precision=highest), None)
    left_sum, unused = lax.scan(add_left, jnp.zeros((ROWS, RANK), jnp.float32), indices)
    left_basis = orthonormal(left_sum)

    def add_right(carry, index):
        return (carry + jnp.dot(merged_of(index).T, left_basis, precision=highest), None)
    new_basis, unused = lax.scan(add_right, jnp.zeros((FF, RANK), jnp.float32), indices)
    approx = jnp.dot(left_basis, new_basis.T, precision=highest) / WORKERS

    def corrected(index):
        return (merged_of(index) - approx).astype(jnp.bfloat16)
    new_feedback = lax.map(corrected, indices)
    return (new_feedback, new_basis)
```

```python
import jax
import jax.numpy as jnp
from jax import lax
from jax.experimental import pallas as pl
from jax.experimental.pallas import tpu as pltpu
from jax.sharding import PartitionSpec as P

MESH = pl.DeviceIdType.MESH

ROWS = 72
FF = 7168
RANK = 32
SIDE = 4
CHIPS = SIDE * SIDE
PLANE = 2 * CHIPS
DEEP = 16
LANES = 128
STRIPS = FF // LANES
QUARTER = STRIPS // 8
EARLY = 4
PAIR = 2
PIECE = PAIR * LANES // DEEP
TILES = ROWS // 8
LOADS = 7
CHUNK = FF // LOADS
WORKERS = 512
EPSILON = 1e-06


def wrap(value, size):
    return jnp.where(value >= size, value - size, value)


def fold(x):
    rows = x.shape[0]
    row = lax.broadcasted_iota(jnp.int32, x.shape, 0)
    lane = lax.broadcasted_iota(jnp.int32, x.shape, 1)
    for step in (1, 2, 4):
        low = (row & step) == 0
        near = (lane & (step * PIECE)) == 0
        up = pltpu.roll(pltpu.roll(x, rows - step, 0), step * PIECE, 1)
        down = pltpu.roll(pltpu.roll(x, step, 0), LANES - step * PIECE, 1)
        x = jnp.where(low & ~near, up, jnp.where(~low & near, down, x))
    return x


def orthonormal(tiles):
    row = lax.broadcasted_iota(jnp.int32, (8, LANES), 0)
    tiles = list(tiles)
    for index in range(RANK):
        own, at = divmod(index, 8)
        vector = jnp.broadcast_to(tiles[own][at : at + 1, :], (8, LANES))
        square = jnp.sum(vector * vector, axis=1, keepdims=True)
        inner = [jnp.sum(t * vector, axis=1, keepdims=True) for t in tiles[own:]]
        scale = lax.rsqrt(square + EPSILON)
        unit = vector * scale
        for later, product in enumerate(inner):
            moved = tiles[own + later] - (product * scale) * unit
            if later == 0:
                moved = jnp.where(row > at, moved, jnp.where(row == at, unit, tiles[own]))
            tiles[own + later] = moved
    return tiles


def kernel(
    g_hbm, f_hbm, b_hbm, out, new_basis,
    g, f, b, m, pr, up_in, down_in, from_below, from_above, strips, second,
    w, a_snd, a_rcv, s_snd, s_rcv, t_snd, t_rcv, zs, zr, pk, zg, nb, lc,
    ld, row_sems, d_s, d_r, p_s, p_r, q_s, q_r, piece_sems, part_sems, n_s, n_r, f_s, f_r,
):
    y = lax.axis_index("local")
    dp = lax.axis_index("dp")
    z, x, core = dp // (2 * SIDE), (dp // 2) % SIDE, dp % 2
    chip = y * SIDE + x
    me = chip * 2 + core
    level = z * (2 * SIDE)
    partner = (y, level + 2 * x + 1 - core)
    first = jnp.where(core == 0, x, y)
    then = jnp.where(core == 0, y, x)

    def at(one, two):
        return (jnp.where(core == 0, two, one), level + 2 * jnp.where(core == 0, one, two) + core)

    def remote(src, dst, send, recv, device):
        return pltpu.make_async_remote_copy(
            src_ref=src, dst_ref=dst, send_sem=send, recv_sem=recv, device_id=device, device_id_type=MESH
        )

    def arrived(sem, ref):
        pltpu.make_async_copy(ref, ref, sem).wait()

    ys = [wrap(y + i, SIDE) for i in range(SIDE)]
    xs = [wrap(x + i, SIDE) for i in range(SIDE)]
    cores = [core, 1 - core]
    far = (0, 1, 2, 1)
    offsets = sorted(
        ((i, j, k) for i in range(SIDE) for j in range(SIDE) for k in range(2) if i + j + k),
        key=lambda o: -(far[o[0]] + far[o[1]]),
    )
    plane = [((ys[i], level + 2 * xs[j] + cores[k]), (ys[i] * SIDE + xs[j]) * 2 + cores[k]) for i, j, k in offsets]
    chips = [((ys[i], level + 2 * xs[j] + core), ys[i] * SIDE + xs[j]) for i, j, k in offsets if k == 0]

    def deep(i):
        peer = wrap(z + i, DEEP)
        return (y, peer * (2 * SIDE) + 2 * x + core), peer

    def chunk(k):
        return pl.ds(k * CHUNK, CHUNK)

    loads = []
    for k in range(LOADS):
        some = []
        for index, (src, dst) in enumerate(((b_hbm, b), (g_hbm, g), (f_hbm, f))):
            copy = pltpu.make_async_copy(src.at[:, chunk(k)], dst.at[:, chunk(k)], ld.at[k, index])
            copy.start()
            some.append(copy)
        loads.append(some)

    barrier = pltpu.get_barrier_semaphore()
    for device, _ in plane:
        pl.semaphore_signal(barrier, inc=1, device_id=device, device_id_type=MESH)

    @pl.loop(1, DEEP)
    def _(i):
        pl.semaphore_signal(barrier, inc=1, device_id=deep(i)[0], device_id_type=MESH)

    total = jnp.zeros((3 * RANK, ROWS), jnp.float32)
    for k in range(LOADS):
        for copy in loads[k]:
            copy.wait()
        basis = b[:, k * CHUNK : (k + 1) * CHUNK]
        high = basis.astype(jnp.bfloat16)
        rest = basis - high.astype(jnp.float32)
        middle = rest.astype(jnp.bfloat16)
        low = (rest - middle.astype(jnp.float32)).astype(jnp.bfloat16)
        parts = jnp.concatenate([high, middle, low], axis=0)
        gk = g[:, k * CHUNK : (k + 1) * CHUNK]
        fk = f[:, k * CHUNK : (k + 1) * CHUNK]
        dims = (((1,), (1,)), ((), ()))
        total += lax.dot_general(parts, gk, dims, preferred_element_type=jnp.float32)
        total += lax.dot_general(parts, fk, dims, preferred_element_type=jnp.float32)
        merged = gk.astype(jnp.float32) + fk.astype(jnp.float32)
        for j in range(CHUNK // LANES):
            m[k * (CHUNK // LANES) + j] = merged[:, j * LANES : (j + 1) * LANES]
    w[...] = jnp.zeros_like(w)
    w[:, :ROWS] = total[2 * RANK :] + total[RANK : 2 * RANK] + total[:RANK]
    left = w[...]
    for k in range(RANK):
        a_snd[k] = left[k : k + 1, :]
    a_rcv[me] = a_snd[me]
    strips[QUARTER] = jnp.zeros((ROWS, LANES), jnp.float32)

    pl.semaphore_wait(barrier, PLANE - 1 + DEEP - 1)

    for device, peer in plane:
        remote(a_snd.at[peer], a_rcv.at[me], row_sems.at[0], row_sems.at[1], device).start()

    spans = ((0, EARLY), (EARLY, QUARTER - EARLY))
    order = [(2, 0), (2, 1), (1, 1), (3, 0), (1, 0), (3, 1), (0, 0), (0, 1)]

    def pair_copy(step, core_to, place):
        ahead, span = order[step]
        start, size = spans[span]
        there = wrap(place + ahead, SIDE) * QUARTER + start
        src, dst = m.at[pl.ds(core_to * (STRIPS // 2) + there, size)], pr.at[pl.ds(there, size)]
        return remote(src, dst, d_s.at[step], d_r.at[step], partner)

    def paired(step):
        pair_copy(step, core, first).wait_recv()
        ahead, span = order[step]
        start, size = spans[span]
        there = wrap(first + ahead, SIDE) * QUARTER + start
        mine = m.at[pl.ds(core * (STRIPS // 2) + there, size)]
        mine[...] = mine[...] + pr[pl.ds(there, size)]
        return mine

    for step in range(8):
        pair_copy(step, 1 - core, then).start()
    above, below = at(wrap(first + 1, SIDE), then), at(wrap(first + 3, SIDE), then)
    upper, lower = pl.ds(EARLY, QUARTER - EARLY), pl.ds(0, EARLY)
    ring = []

    def pass_round(src, dst, device):
        index = len(ring)
        copy = remote(src, dst, p_s.at[index], p_r.at[index], device)
        copy.start()
        ring.append(copy)

    pass_round(paired(0), up_in, above)
    pass_round(paired(1), down_in, below)
    pass_round(paired(2), from_below.at[upper], above)
    pass_round(paired(3), from_above.at[lower], below)
    mine = paired(4)
    ring[0].wait_recv()
    mine[...] = mine[...] + up_in[...]
    pass_round(mine, from_below.at[lower], above)
    mine = paired(5)
    ring[1].wait_recv()
    mine[...] = mine[...] + down_in[...]
    pass_round(mine, from_above.at[upper], below)

    arrived(row_sems.at[1], a_rcv.at[pl.ds(0, PLANE - 1)])
    own_row = jnp.sum(a_rcv[...], axis=0)
    s_snd[0] = own_row
    s_rcv[z] = own_row

    @pl.loop(1, DEEP)
    def _(i):
        device, _ = deep(i)
        remote(s_snd.at[0], s_rcv.at[z], row_sems.at[2], row_sems.at[3], device).start()

    paired(6)
    paired(7)
    for index in (2, 3, 4, 5):
        ring[index].wait_recv()
    base = core * (STRIPS // 2) + first * QUARTER
    for t in range(QUARTER):
        strips[t] = m[base + t] + (from_below[t] + from_above[t])

    def second_copy(ahead, slot):
        two = wrap(then + ahead, SIDE)
        src = strips.at[pl.ds(PAIR * two, PAIR)]
        return remote(src, second.at[slot], q_s.at[ahead - 1], q_r.at[ahead - 1], at(first, two))

    for ahead in (2, 1, 3):
        second_copy(ahead, ahead - 1).start()

    arrived(row_sems.at[3], s_rcv.at[pl.ds(0, DEEP - 1)])
    whole_row = jnp.sum(s_rcv[...], axis=0)
    t_snd[0] = whole_row
    t_rcv[me] = whole_row
    for device, _ in plane:
        remote(t_snd.at[0], t_rcv.at[me], row_sems.at[4], row_sems.at[5], device).start()

    for ahead in (1, 3, 2):
        second_copy(ahead, ahead - 1).wait_recv()
    for t in range(PAIR):
        strip = (strips[PAIR * then + t] + second[0, t]) + (second[1, t] + second[2, t])
        folded = fold(strip)
        for i in range(TILES):
            for p in range(8):
                zs[8 * t + p, i] = folded[8 * i + p : 8 * i + p + 1, :]
    zr[z] = zs[z]

    @pl.loop(1, DEEP)
    def _(i):
        device, peer = deep(i)
        remote(zs.at[peer], zr.at[z], piece_sems.at[0], piece_sems.at[1], device).start()

    arrived(row_sems.at[5], t_rcv.at[pl.ds(0, PLANE - 1)])
    tiles = [jnp.concatenate([t_rcv[8 * t + k] for k in range(8)], axis=0) for t in range(RANK // 8)]
    basis = jnp.concatenate(orthonormal(tiles), axis=0)
    scaled = basis * (1.0 / WORKERS)
    high = scaled.astype(jnp.bfloat16).astype(jnp.float32)
    split = jnp.concatenate([high, high, scaled - high, jnp.zeros((RANK, LANES), jnp.float32)], axis=0)
    lc[...] = jnp.transpose(split)[:ROWS].astype(jnp.bfloat16)

    arrived(piece_sems.at[1], zr.at[pl.ds(0, DEEP - 1)])
    piece = jnp.sum(zr[...], axis=0)
    row = lax.broadcasted_iota(jnp.int32, (8, LANES), 0)
    lane = lax.broadcasted_iota(jnp.int32, (8, LANES), 1)
    diagonal = (lane // PIECE) == row
    spread = [jnp.where(diagonal, jnp.broadcast_to(piece[i], (8, LANES)), 0.0) for i in range(TILES)]
    spread.append(jnp.zeros((LANES - ROWS, LANES), jnp.float32))
    part = jnp.dot(
        basis, jnp.concatenate(spread, axis=0), precision=lax.Precision.HIGHEST, preferred_element_type=jnp.float32
    )
    for step in (1, 2, 4):
        part = part + pltpu.roll(part, step * PIECE, 1)
    for k in range(RANK // 8):
        packed = jnp.where(diagonal, part[8 * k : 8 * k + 8], 0.0)
        pk[k] = jnp.sum(packed, axis=0, keepdims=True)
        zg[k, z] = pk[k]

    @pl.loop(1, DEEP)
    def _(i):
        device, _ = deep(i)
        remote(pk, zg.at[:, z], part_sems.at[0], part_sems.at[1], device).start()

    arrived(part_sems.at[1], zg.at[:, pl.ds(0, DEEP - 1)])

    def block_of(chip_at, of_core):
        one = jnp.where(of_core == 0, chip_at % SIDE, chip_at // SIDE)
        two = jnp.where(of_core == 0, chip_at // SIDE, chip_at % SIDE)
        columns = pl.ds(pl.multiple_of(two * (PAIR * LANES), LANES), PAIR * LANES)
        return nb.at[of_core * SIDE + one, :, columns]

    def spread_block(device, chip_at, slot):
        return remote(block_of(chip, core), block_of(slot, core), n_s.at[chip_at], n_r.at[slot], device)

    def pass_on(chip_at, of_core):
        block = block_of(chip_at, of_core)
        return remote(block, block, f_s.at[chip_at], f_r.at[chip_at], partner)

    for t in range(PAIR):
        rows = [zg[k, 8 * t + p] for k in range(RANK // 8) for p in range(8)]
        columns = pl.ds(pl.multiple_of(then * (PAIR * LANES) + t * LANES, LANES), LANES)
        nb[core * SIDE + first, :, columns] = fold(jnp.concatenate(rows, axis=0))
    for device, chip_at in chips:
        spread_block(device, chip_at, chip).start()
    pass_on(chip, core).start()

    width = QUARTER * LANES

    def finish(half, quarter):
        here = pl.ds(pl.multiple_of((half * SIDE + quarter) * width, LANES), width)
        new = nb[half * SIDE + quarter, :, :width]
        new_basis[:, here] = new
        high = new.astype(jnp.bfloat16)
        low = (new - high.astype(jnp.float32)).astype(jnp.bfloat16)
        parts = jnp.concatenate([high, low, high, jnp.zeros_like(high)], axis=0)
        approx = jnp.dot(lc[...], parts, preferred_element_type=jnp.float32)
        merged = g[:, here].astype(jnp.float32) + f[:, here].astype(jnp.float32)
        out[:, here] = (merged - approx).astype(jnp.bfloat16)

    for device, chip_at in reversed(chips):
        spread_block(device, chip_at, chip_at).wait_recv()
        pass_on(chip_at, core).start()

    @pl.loop(0, SIDE)
    def _(quarter):
        finish(core, quarter)

    @pl.loop(0, CHIPS)
    def _(chip_at):
        pass_on(chip_at, 1 - core).wait_recv()

    @pl.loop(0, SIDE)
    def _(quarter):
        finish(1 - core, quarter)

    arrived(row_sems.at[0], a_rcv.at[pl.ds(0, PLANE - 1)])
    arrived(row_sems.at[2], s_rcv.at[pl.ds(0, DEEP - 1)])
    arrived(row_sems.at[4], t_rcv.at[pl.ds(0, PLANE - 1)])
    arrived(piece_sems.at[0], zr.at[pl.ds(0, DEEP - 1)])
    arrived(part_sems.at[0], zg.at[:, pl.ds(0, DEEP - 1)])
    for step in range(8):
        pair_copy(step, 1 - core, then).wait_send()
    for copy in ring:
        copy.wait_send()
    for ahead in (1, 2, 3):
        second_copy(ahead, ahead - 1).wait_send()
    for device, chip_at in chips:
        spread_block(device, chip_at, chip).wait_send()

    @pl.loop(0, CHIPS)
    def _(chip_at):
        pass_on(chip_at, core).wait_send()


def write(feedback, basis, feedback_out, basis_out, sems):
    copies = [
        pltpu.make_async_copy(feedback, feedback_out, sems.at[0]),
        pltpu.make_async_copy(basis, basis_out, sems.at[1]),
    ]
    for copy in copies:
        copy.start()
    for copy in copies:
        copy.wait()


def body(gradient, feedback, basis_in):
    f32, bf16 = jnp.float32, jnp.bfloat16
    dma = pltpu.SemaphoreType.DMA
    shapes = (jax.ShapeDtypeStruct((ROWS, FF), bf16), jax.ShapeDtypeStruct((RANK, FF), f32))
    new_feedback, new_basis = pl.pallas_call(
        kernel,
        out_shape=(pltpu.VMEM((ROWS, FF), bf16), pltpu.VMEM((RANK, FF), f32)),
        in_specs=[pl.BlockSpec(memory_space=pltpu.HBM)] * 3,
        out_specs=(pl.BlockSpec(memory_space=pltpu.VMEM),) * 2,
        scratch_shapes=[
            pltpu.VMEM((ROWS, FF), bf16),
            pltpu.VMEM((ROWS, FF), bf16),
            pltpu.VMEM((RANK, FF), f32),
            pltpu.VMEM((STRIPS, ROWS, LANES), f32),
            pltpu.VMEM((STRIPS // 2, ROWS, LANES), f32),
            pltpu.VMEM((EARLY, ROWS, LANES), f32),
            pltpu.VMEM((QUARTER - EARLY, ROWS, LANES), f32),
            pltpu.VMEM((QUARTER, ROWS, LANES), f32),
            pltpu.VMEM((QUARTER, ROWS, LANES), f32),
            pltpu.VMEM((SIDE * PAIR, ROWS, LANES), f32),
            pltpu.VMEM((SIDE - 1, PAIR, ROWS, LANES), f32),
            pltpu.VMEM((RANK, LANES), f32),
            pltpu.VMEM((PLANE, 1, LANES), f32),
            pltpu.VMEM((PLANE, 1, LANES), f32),
            pltpu.VMEM((1, 1, LANES), f32),
            pltpu.VMEM((DEEP, 1, LANES), f32),
            pltpu.VMEM((1, 1, LANES), f32),
            pltpu.VMEM((PLANE, 1, LANES), f32),
            pltpu.VMEM((DEEP, TILES, 1, LANES), f32),
            pltpu.VMEM((DEEP, TILES, 1, LANES), f32),
            pltpu.VMEM((RANK // 8, 1, LANES), f32),
            pltpu.VMEM((RANK // 8, DEEP, 1, LANES), f32),
            pltpu.VMEM((2 * SIDE, RANK, SIDE * PAIR * LANES), f32),
            pltpu.VMEM((ROWS, LANES), bf16),
            dma((LOADS, 3)),
            dma((6,)),
            dma((8,)), dma((8,)),
            dma((6,)), dma((6,)),
            dma((SIDE - 1,)), dma((SIDE - 1,)),
            dma((2,)),
            dma((2,)),
            dma((CHIPS,)), dma((CHIPS,)),
            dma((CHIPS,)), dma((CHIPS,)),
        ],
        compiler_params=pltpu.CompilerParams(
            collective_id=0, has_side_effects=True, vmem_limit_bytes=65_093_632
        ),
        name="powersgd_step",
    )(gradient[0], feedback[0], basis_in.T)
    new_feedback, new_basis = pl.pallas_call(
        write,
        out_shape=shapes,
        in_specs=[pl.BlockSpec(memory_space=pl.ANY)] * 2,
        out_specs=(pl.BlockSpec(memory_space=pltpu.HBM),) * 2,
        scratch_shapes=[dma((2,))],
        compiler_params=pltpu.CompilerParams(vmem_limit_bytes=4 * 1024 * 1024),
        name="write_out",
    )(*(pltpu.with_memory_space_constraint(x, pltpu.VMEM) for x in (new_feedback, new_basis)))
    return new_feedback[None], new_basis.T


def solution(mesh):
    spec = P(("local", "dp"), None, None)
    return jax.shard_map(
        body, mesh=mesh, in_specs=(spec, spec, P()), out_specs=(spec, P()), check_vma=False
    )
```

```python
import jax
import jax.numpy as jnp
from jax import lax
from jax.experimental import pallas as pl
from jax.experimental.pallas import tpu as pltpu
from jax.sharding import PartitionSpec as P

MESH = pl.DeviceIdType.MESH

ROWS = 72
FF = 7168
RANK = 32
SIDE = 4
CHIPS = SIDE * SIDE
PLANE = 2 * CHIPS
DEEP = 16
REACH = DEEP // 4
LANES = 128
STRIPS = FF // LANES
QUARTER = STRIPS // 8
EARLY = 4
PAIR = 2
PIECE = PAIR * LANES // DEEP
TILES = ROWS // 8
LOADS = 7
CHUNK = FF // LOADS
WORKERS = 512
EPSILON = 1e-06


def wrap(value, size):
    return jnp.where(value >= size, value - size, value)


def fold(x):
    rows = x.shape[0]
    row = lax.broadcasted_iota(jnp.int32, x.shape, 0)
    lane = lax.broadcasted_iota(jnp.int32, x.shape, 1)
    for step in (1, 2, 4):
        low = (row & step) == 0
        near = (lane & (step * PIECE)) == 0
        up = pltpu.roll(pltpu.roll(x, rows - step, 0), step * PIECE, 1)
        down = pltpu.roll(pltpu.roll(x, step, 0), LANES - step * PIECE, 1)
        x = jnp.where(low & ~near, up, jnp.where(~low & near, down, x))
    return x


def orthonormal(tiles):
    row = lax.broadcasted_iota(jnp.int32, (8, LANES), 0)
    tiles = list(tiles)
    for index in range(RANK):
        own, at = divmod(index, 8)
        vector = jnp.broadcast_to(tiles[own][at : at + 1, :], (8, LANES))
        square = jnp.sum(vector * vector, axis=1, keepdims=True)
        inner = [jnp.sum(t * vector, axis=1, keepdims=True) for t in tiles[own:]]
        scale = lax.rsqrt(square + EPSILON)
        unit = vector * scale
        for later, product in enumerate(inner):
            moved = tiles[own + later] - (product * scale) * unit
            if later == 0:
                moved = jnp.where(row > at, moved, jnp.where(row == at, unit, tiles[own]))
            tiles[own + later] = moved
    return tiles


def kernel(
    g_hbm, f_hbm, b_hbm, out, new_basis,
    g, f, b, m, pr, up_in, down_in, from_below, from_above, strips, second,
    w, a_snd, a_rcv, s_snd, s_rcv, t_snd, t_rcv, zs, zr, pk, zg, nb, lc,
    ld, row_sems, d_s, d_r, p_s, p_r, q_s, q_r, piece_sems, part_sems, n_s, n_r, f_s, f_r, reach,
):
    y = lax.axis_index("local")
    dp = lax.axis_index("dp")
    z, x, core = dp // (2 * SIDE), (dp // 2) % SIDE, dp % 2
    chip = y * SIDE + x
    me = chip * 2 + core
    level = z * (2 * SIDE)
    partner = (y, level + 2 * x + 1 - core)
    first = jnp.where(core == 0, x, y)
    then = jnp.where(core == 0, y, x)

    def at(one, two):
        return (jnp.where(core == 0, two, one), level + 2 * jnp.where(core == 0, one, two) + core)

    def remote(src, dst, send, recv, device):
        return pltpu.make_async_remote_copy(
            src_ref=src, dst_ref=dst, send_sem=send, recv_sem=recv, device_id=device, device_id_type=MESH
        )

    def arrived(sem, ref):
        pltpu.make_async_copy(ref, ref, sem).wait()

    ys = [wrap(y + i, SIDE) for i in range(SIDE)]
    xs = [wrap(x + i, SIDE) for i in range(SIDE)]
    cores = [core, 1 - core]
    far = (0, 1, 2, 1)
    offsets = sorted(
        ((i, j, k) for i in range(SIDE) for j in range(SIDE) for k in range(2) if i + j + k),
        key=lambda o: -(far[o[0]] + far[o[1]]),
    )
    plane = [((ys[i], level + 2 * xs[j] + cores[k]), (ys[i] * SIDE + xs[j]) * 2 + cores[k]) for i, j, k in offsets]
    chips = [((ys[i], level + 2 * xs[j] + core), ys[i] * SIDE + xs[j]) for i, j, k in offsets if k == 0]

    def deep(i):
        peer = wrap(z + i, DEEP)
        return (y, peer * (2 * SIDE) + 2 * x + core), peer

    def chunk(k):
        return pl.ds(k * CHUNK, CHUNK)

    loads = []
    for k in range(LOADS):
        some = []
        for index, (src, dst) in enumerate(((b_hbm, b), (g_hbm, g), (f_hbm, f))):
            copy = pltpu.make_async_copy(src.at[:, chunk(k)], dst.at[:, chunk(k)], ld.at[k, index])
            copy.start()
            some.append(copy)
        loads.append(some)

    barrier = pltpu.get_barrier_semaphore()
    for device, _ in plane:
        pl.semaphore_signal(barrier, inc=1, device_id=device, device_id_type=MESH)

    for i in range(1, REACH + 1):
        for ahead in (i, DEEP - i):
            pl.semaphore_signal(barrier, inc=1, device_id=deep(ahead)[0], device_id_type=MESH)

    total = jnp.zeros((3 * RANK, ROWS), jnp.float32)
    for k in range(LOADS):
        for copy in loads[k]:
            copy.wait()
        basis = b[:, k * CHUNK : (k + 1) * CHUNK]
        high = basis.astype(jnp.bfloat16)
        rest = basis - high.astype(jnp.float32)
        middle = rest.astype(jnp.bfloat16)
        low = (rest - middle.astype(jnp.float32)).astype(jnp.bfloat16)
        parts = jnp.concatenate([high, middle, low], axis=0)
        gk = g[:, k * CHUNK : (k + 1) * CHUNK]
        fk = f[:, k * CHUNK : (k + 1) * CHUNK]
        dims = (((1,), (1,)), ((), ()))
        total += lax.dot_general(parts, gk, dims, preferred_element_type=jnp.float32)
        total += lax.dot_general(parts, fk, dims, preferred_element_type=jnp.float32)
        merged = gk.astype(jnp.float32) + fk.astype(jnp.float32)
        for j in range(CHUNK // LANES):
            m[k * (CHUNK // LANES) + j] = merged[:, j * LANES : (j + 1) * LANES]
    w[...] = jnp.zeros_like(w)
    w[:, :ROWS] = total[2 * RANK :] + total[RANK : 2 * RANK] + total[:RANK]
    left = w[...]
    for k in range(RANK):
        a_snd[k] = left[k : k + 1, :]
    a_rcv[me] = a_snd[me]
    strips[QUARTER] = jnp.zeros((ROWS, LANES), jnp.float32)

    pl.semaphore_wait(barrier, PLANE - 1 + 2 * REACH)
    for ahead in (REACH, DEEP - REACH):
        pl.semaphore_signal(reach, inc=1, device_id=deep(ahead)[0], device_id_type=MESH)

    spans = ((0, EARLY), (EARLY, QUARTER - EARLY))
    order = [(2, 0), (2, 1), (1, 1), (3, 0), (1, 0), (3, 1), (0, 0), (0, 1)]

    def pair_copy(step, core_to, place):
        ahead, span = order[step]
        start, size = spans[span]
        there = wrap(place + ahead, SIDE) * QUARTER + start
        src, dst = m.at[pl.ds(core_to * (STRIPS // 2) + there, size)], pr.at[pl.ds(there, size)]
        return remote(src, dst, d_s.at[step], d_r.at[step], partner)

    def paired(step):
        pair_copy(step, core, first).wait_recv()
        ahead, span = order[step]
        start, size = spans[span]
        there = wrap(first + ahead, SIDE) * QUARTER + start
        mine = m.at[pl.ds(core * (STRIPS // 2) + there, size)]
        mine[...] = mine[...] + pr[pl.ds(there, size)]
        return mine

    for step in range(8):
        pair_copy(step, 1 - core, then).start()

    for device, peer in plane:
        remote(a_snd.at[peer], a_rcv.at[me], row_sems.at[0], row_sems.at[1], device).start()

    above, below = at(wrap(first + 1, SIDE), then), at(wrap(first + 3, SIDE), then)
    upper, lower = pl.ds(EARLY, QUARTER - EARLY), pl.ds(0, EARLY)
    ring = []

    def pass_round(src, dst, device):
        index = len(ring)
        copy = remote(src, dst, p_s.at[index], p_r.at[index], device)
        copy.start()
        ring.append(copy)

    pass_round(paired(0), up_in, above)
    pass_round(paired(1), down_in, below)
    pass_round(paired(2), from_below.at[upper], above)
    pass_round(paired(3), from_above.at[lower], below)
    mine = paired(4)
    ring[0].wait_recv()
    mine[...] = mine[...] + up_in[...]
    pass_round(mine, from_below.at[lower], above)
    mine = paired(5)
    ring[1].wait_recv()
    mine[...] = mine[...] + down_in[...]
    pass_round(mine, from_above.at[upper], below)

    pl.semaphore_wait(reach, 2)
    arrived(row_sems.at[1], a_rcv.at[pl.ds(0, PLANE - 1)])
    own_row = jnp.sum(a_rcv[...], axis=0)
    s_snd[0] = own_row
    s_rcv[z] = own_row

    @pl.loop(1, DEEP)
    def _(i):
        device, _ = deep(i)
        remote(s_snd.at[0], s_rcv.at[z], row_sems.at[2], row_sems.at[3], device).start()

    paired(6)
    paired(7)
    for index in (2, 3, 4, 5):
        ring[index].wait_recv()
    base = core * (STRIPS // 2) + first * QUARTER
    for t in range(QUARTER):
        strips[t] = m[base + t] + (from_below[t] + from_above[t])

    def second_copy(ahead, slot):
        two = wrap(then + ahead, SIDE)
        src = strips.at[pl.ds(PAIR * two, PAIR)]
        return remote(src, second.at[slot], q_s.at[ahead - 1], q_r.at[ahead - 1], at(first, two))

    for ahead in (2, 1, 3):
        second_copy(ahead, ahead - 1).start()

    arrived(row_sems.at[3], s_rcv.at[pl.ds(0, DEEP - 1)])
    whole_row = jnp.sum(s_rcv[...], axis=0)
    t_snd[0] = whole_row
    t_rcv[me] = whole_row
    for device, _ in plane:
        remote(t_snd.at[0], t_rcv.at[me], row_sems.at[4], row_sems.at[5], device).start()

    for ahead in (1, 3, 2):
        second_copy(ahead, ahead - 1).wait_recv()
    for t in range(PAIR):
        strip = (strips[PAIR * then + t] + second[0, t]) + (second[1, t] + second[2, t])
        folded = fold(strip)
        for i in range(TILES):
            for p in range(8):
                zs[8 * t + p, i] = folded[8 * i + p : 8 * i + p + 1, :]
    zr[z] = zs[z]

    @pl.loop(1, DEEP)
    def _(i):
        device, peer = deep(i)
        remote(zs.at[peer], zr.at[z], piece_sems.at[0], piece_sems.at[1], device).start()

    arrived(row_sems.at[5], t_rcv.at[pl.ds(0, PLANE - 1)])
    tiles = [jnp.concatenate([t_rcv[8 * t + k] for k in range(8)], axis=0) for t in range(RANK // 8)]
    basis = jnp.concatenate(orthonormal(tiles), axis=0)
    scaled = basis * (1.0 / WORKERS)
    high = scaled.astype(jnp.bfloat16).astype(jnp.float32)
    split = jnp.concatenate([high, high, scaled - high, jnp.zeros((RANK, LANES), jnp.float32)], axis=0)
    lc[...] = jnp.transpose(split)[:ROWS].astype(jnp.bfloat16)

    arrived(piece_sems.at[1], zr.at[pl.ds(0, DEEP - 1)])
    piece = jnp.sum(zr[...], axis=0)
    row = lax.broadcasted_iota(jnp.int32, (8, LANES), 0)
    lane = lax.broadcasted_iota(jnp.int32, (8, LANES), 1)
    diagonal = (lane // PIECE) == row
    spread = [jnp.where(diagonal, jnp.broadcast_to(piece[i], (8, LANES)), 0.0) for i in range(TILES)]
    spread.append(jnp.zeros((LANES - ROWS, LANES), jnp.float32))
    part = jnp.dot(
        basis, jnp.concatenate(spread, axis=0), precision=lax.Precision.HIGHEST, preferred_element_type=jnp.float32
    )
    for step in (1, 2, 4):
        part = part + pltpu.roll(part, step * PIECE, 1)
    for k in range(RANK // 8):
        packed = jnp.where(diagonal, part[8 * k : 8 * k + 8], 0.0)
        pk[k] = jnp.sum(packed, axis=0, keepdims=True)
        zg[z, k] = pk[k]

    @pl.loop(1, DEEP)
    def _(i):
        device, _ = deep(i)
        remote(pk, zg.at[z], part_sems.at[0], part_sems.at[1], device).start()

    arrived(part_sems.at[1], zg.at[pl.ds(0, DEEP - 1)])

    def block_of(chip_at, of_core):
        one = jnp.where(of_core == 0, chip_at % SIDE, chip_at // SIDE)
        two = jnp.where(of_core == 0, chip_at // SIDE, chip_at % SIDE)
        return nb.at[of_core * SIDE + one, two]

    def spread_block(device, chip_at, slot):
        return remote(block_of(chip, core), block_of(slot, core), n_s.at[chip_at], n_r.at[slot], device)

    def pass_on(chip_at, of_core):
        block = block_of(chip_at, of_core)
        return remote(block, block, f_s.at[chip_at], f_r.at[chip_at], partner)

    for t in range(PAIR):
        rows = [zg[8 * t + p, k] for k in range(RANK // 8) for p in range(8)]
        nb[core * SIDE + first, then, :, t * LANES : (t + 1) * LANES] = fold(jnp.concatenate(rows, axis=0))
    for device, chip_at in chips:
        spread_block(device, chip_at, chip).start()
    pass_on(chip, core).start()

    width = QUARTER * LANES

    def finish(half, quarter):
        here = pl.ds(pl.multiple_of((half * SIDE + quarter) * width, LANES), width)
        new = jnp.concatenate([nb[half * SIDE + quarter, two] for two in range(SIDE)], axis=1)[:, :width]
        new_basis[:, here] = new
        high = new.astype(jnp.bfloat16)
        low = (new - high.astype(jnp.float32)).astype(jnp.bfloat16)
        parts = jnp.concatenate([high, low, high, jnp.zeros_like(high)], axis=0)
        approx = jnp.dot(lc[...], parts, preferred_element_type=jnp.float32)
        merged = g[:, here].astype(jnp.float32) + f[:, here].astype(jnp.float32)
        out[:, here] = (merged - approx).astype(jnp.bfloat16)

    for device, chip_at in reversed(chips):
        spread_block(device, chip_at, chip_at).wait_recv()
        pass_on(chip_at, core).start()

    @pl.loop(0, SIDE)
    def _(quarter):
        finish(core, quarter)

    @pl.loop(0, SIDE)
    def _(quarter):
        for two in range(SIDE):
            chip_at = jnp.where(core == 1, two * SIDE + quarter, quarter * SIDE + two)
            pass_on(chip_at, 1 - core).wait_recv()
        finish(1 - core, quarter)

    arrived(row_sems.at[0], a_rcv.at[pl.ds(0, PLANE - 1)])
    arrived(row_sems.at[2], s_rcv.at[pl.ds(0, DEEP - 1)])
    arrived(row_sems.at[4], t_rcv.at[pl.ds(0, PLANE - 1)])
    arrived(piece_sems.at[0], zr.at[pl.ds(0, DEEP - 1)])
    arrived(part_sems.at[0], zg.at[pl.ds(0, DEEP - 1)])
    for step in range(8):
        pair_copy(step, 1 - core, then).wait_send()
    for copy in ring:
        copy.wait_send()
    for ahead in (1, 2, 3):
        second_copy(ahead, ahead - 1).wait_send()
    for device, chip_at in chips:
        spread_block(device, chip_at, chip).wait_send()

    @pl.loop(0, CHIPS)
    def _(chip_at):
        pass_on(chip_at, core).wait_send()


def write(feedback, basis, feedback_out, basis_out, sems):
    copies = [
        pltpu.make_async_copy(feedback, feedback_out, sems.at[0]),
        pltpu.make_async_copy(basis, basis_out, sems.at[1]),
    ]
    for copy in copies:
        copy.start()
    for copy in copies:
        copy.wait()


def body(gradient, feedback, basis_in):
    f32, bf16 = jnp.float32, jnp.bfloat16
    dma = pltpu.SemaphoreType.DMA
    shapes = (jax.ShapeDtypeStruct((ROWS, FF), bf16), jax.ShapeDtypeStruct((RANK, FF), f32))
    new_feedback, new_basis = pl.pallas_call(
        kernel,
        out_shape=(pltpu.VMEM((ROWS, FF), bf16), pltpu.VMEM((RANK, FF), f32)),
        in_specs=[pl.BlockSpec(memory_space=pltpu.HBM)] * 3,
        out_specs=(pl.BlockSpec(memory_space=pltpu.VMEM),) * 2,
        scratch_shapes=[
            pltpu.VMEM((ROWS, FF), bf16),
            pltpu.VMEM((ROWS, FF), bf16),
            pltpu.VMEM((RANK, FF), f32),
            pltpu.VMEM((STRIPS, ROWS, LANES), f32),
            pltpu.VMEM((STRIPS // 2, ROWS, LANES), f32),
            pltpu.VMEM((EARLY, ROWS, LANES), f32),
            pltpu.VMEM((QUARTER - EARLY, ROWS, LANES), f32),
            pltpu.VMEM((QUARTER, ROWS, LANES), f32),
            pltpu.VMEM((QUARTER, ROWS, LANES), f32),
            pltpu.VMEM((SIDE * PAIR, ROWS, LANES), f32),
            pltpu.VMEM((SIDE - 1, PAIR, ROWS, LANES), f32),
            pltpu.VMEM((RANK, LANES), f32),
            pltpu.VMEM((PLANE, 1, LANES), f32),
            pltpu.VMEM((PLANE, 1, LANES), f32),
            pltpu.VMEM((1, 1, LANES), f32),
            pltpu.VMEM((DEEP, 1, LANES), f32),
            pltpu.VMEM((1, 1, LANES), f32),
            pltpu.VMEM((PLANE, 1, LANES), f32),
            pltpu.VMEM((DEEP, TILES, 1, LANES), f32),
            pltpu.VMEM((DEEP, TILES, 1, LANES), f32),
            pltpu.VMEM((RANK // 8, 1, LANES), f32),
            pltpu.VMEM((DEEP, RANK // 8, 1, LANES), f32),
            pltpu.VMEM((2 * SIDE, SIDE, RANK, PAIR * LANES), f32),
            pltpu.VMEM((ROWS, LANES), bf16),
            dma((LOADS, 3)),
            dma((6,)),
            dma((8,)), dma((8,)),
            dma((6,)), dma((6,)),
            dma((SIDE - 1,)), dma((SIDE - 1,)),
            dma((2,)),
            dma((2,)),
            dma((CHIPS,)), dma((CHIPS,)),
            dma((CHIPS,)), dma((CHIPS,)),
            pltpu.SemaphoreType.REGULAR,
        ],
        compiler_params=pltpu.CompilerParams(
            collective_id=0, has_side_effects=True, vmem_limit_bytes=65_093_632
        ),
        name="powersgd_step",
    )(gradient[0], feedback[0], basis_in.T)
    new_feedback, new_basis = pl.pallas_call(
        write,
        out_shape=shapes,
        in_specs=[pl.BlockSpec(memory_space=pl.ANY)] * 2,
        out_specs=(pl.BlockSpec(memory_space=pltpu.HBM),) * 2,
        scratch_shapes=[dma((2,))],
        compiler_params=pltpu.CompilerParams(vmem_limit_bytes=4 * 1024 * 1024),
        name="write_out",
    )(*(pltpu.with_memory_space_constraint(x, pltpu.VMEM) for x in (new_feedback, new_basis)))
    return new_feedback[None], new_basis.T


def solution(mesh):
    spec = P(("local", "dp"), None, None)
    return jax.shard_map(
        body, mesh=mesh, in_specs=(spec, spec, P()), out_specs=(spec, P()), check_vma=False
    )
```

```python
import jax
import jax.numpy as jnp
from jax import lax
from jax.experimental import pallas as pl
from jax.experimental.pallas import tpu as pltpu
from jax.sharding import PartitionSpec as P

MESH = pl.DeviceIdType.MESH

ROWS = 72
FF = 7168
RANK = 32
SIDE = 4
CHIPS = SIDE * SIDE
PLANE = 2 * CHIPS
DEEP = 16
REACH = DEEP // 4
LANES = 128
STRIPS = FF // LANES
QUARTER = STRIPS // 8
EARLY = 4
PAIR = 2
PIECE = PAIR * LANES // DEEP
TILES = ROWS // 8
LOADS = 7
CHUNK = FF // LOADS
WORKERS = 512
EPSILON = 1e-06


def wrap(value, size):
    return jnp.where(value >= size, value - size, value)


def fold(x):
    rows = x.shape[0]
    row = lax.broadcasted_iota(jnp.int32, x.shape, 0)
    lane = lax.broadcasted_iota(jnp.int32, x.shape, 1)
    for step in (1, 2, 4):
        low = (row & step) == 0
        near = (lane & (step * PIECE)) == 0
        up = pltpu.roll(pltpu.roll(x, rows - step, 0), step * PIECE, 1)
        down = pltpu.roll(pltpu.roll(x, step, 0), LANES - step * PIECE, 1)
        x = jnp.where(low & ~near, up, jnp.where(~low & near, down, x))
    return x


def orthonormal(tiles):
    row = lax.broadcasted_iota(jnp.int32, (8, LANES), 0)
    tiles = list(tiles)
    for index in range(RANK):
        own, at = divmod(index, 8)
        vector = jnp.broadcast_to(tiles[own][at : at + 1, :], (8, LANES))
        square = jnp.sum(vector * vector, axis=1, keepdims=True)
        inner = [jnp.sum(t * vector, axis=1, keepdims=True) for t in tiles[own:]]
        scale = lax.rsqrt(square + EPSILON)
        unit = vector * scale
        for later, product in enumerate(inner):
            moved = tiles[own + later] - (product * scale) * unit
            if later == 0:
                moved = jnp.where(row > at, moved, jnp.where(row == at, unit, tiles[own]))
            tiles[own + later] = moved
    return tiles


def kernel(
    g_hbm, f_hbm, b_hbm, out, new_basis,
    g, f, b, m, pr, up_in, down_in, from_below, from_above, strips, second,
    w, a_snd, a_rcv, s_snd, s_rcv, t_snd, t_rcv, zs, zr, pk, zg, nb, lc,
    ld, row_sems, d_s, d_r, p_s, p_r, q_s, q_r, piece_sems, part_sems, n_s, n_r, f_s, f_r, reach,
):
    y = lax.axis_index("local")
    dp = lax.axis_index("dp")
    z, x, core = dp // (2 * SIDE), (dp // 2) % SIDE, dp % 2
    chip = y * SIDE + x
    me = chip * 2 + core
    level = z * (2 * SIDE)
    partner = (y, level + 2 * x + 1 - core)
    first = jnp.where(core == 0, x, y)
    then = jnp.where(core == 0, y, x)

    def at(one, two):
        return (jnp.where(core == 0, two, one), level + 2 * jnp.where(core == 0, one, two) + core)

    def remote(src, dst, send, recv, device):
        return pltpu.make_async_remote_copy(
            src_ref=src, dst_ref=dst, send_sem=send, recv_sem=recv, device_id=device, device_id_type=MESH
        )

    def arrived(sem, ref):
        pltpu.make_async_copy(ref, ref, sem).wait()

    ys = [wrap(y + i, SIDE) for i in range(SIDE)]
    xs = [wrap(x + i, SIDE) for i in range(SIDE)]
    cores = [core, 1 - core]
    far = (0, 1, 2, 1)
    offsets = sorted(
        ((i, j, k) for i in range(SIDE) for j in range(SIDE) for k in range(2) if i + j + k),
        key=lambda o: -(far[o[0]] + far[o[1]]),
    )
    plane = [((ys[i], level + 2 * xs[j] + cores[k]), (ys[i] * SIDE + xs[j]) * 2 + cores[k]) for i, j, k in offsets]
    chips = [((ys[i], level + 2 * xs[j] + core), ys[i] * SIDE + xs[j]) for i, j, k in offsets if k == 0]

    def deep(i):
        peer = wrap(z + i, DEEP)
        return (y, peer * (2 * SIDE) + 2 * x + core), peer

    planes = [deep(i) for i in sorted(range(1, DEEP), key=lambda i: -min(i, DEEP - i))]

    def chunk(k):
        return pl.ds(k * CHUNK, CHUNK)

    loads = []
    for k in range(LOADS):
        some = []
        for index, (src, dst) in enumerate(((b_hbm, b), (g_hbm, g), (f_hbm, f))):
            copy = pltpu.make_async_copy(src.at[:, chunk(k)], dst.at[:, chunk(k)], ld.at[k, index])
            copy.start()
            some.append(copy)
        loads.append(some)

    barrier = pltpu.get_barrier_semaphore()
    for device, _ in plane:
        pl.semaphore_signal(barrier, inc=1, device_id=device, device_id_type=MESH)

    for i in range(1, REACH + 1):
        for ahead in (i, DEEP - i):
            pl.semaphore_signal(barrier, inc=1, device_id=deep(ahead)[0], device_id_type=MESH)

    total = jnp.zeros((3 * RANK, ROWS), jnp.float32)
    for k in range(LOADS):
        for copy in loads[k]:
            copy.wait()
        basis = b[:, k * CHUNK : (k + 1) * CHUNK]
        high = basis.astype(jnp.bfloat16)
        rest = basis - high.astype(jnp.float32)
        middle = rest.astype(jnp.bfloat16)
        low = (rest - middle.astype(jnp.float32)).astype(jnp.bfloat16)
        parts = jnp.concatenate([high, middle, low], axis=0)
        gk = g[:, k * CHUNK : (k + 1) * CHUNK]
        fk = f[:, k * CHUNK : (k + 1) * CHUNK]
        dims = (((1,), (1,)), ((), ()))
        total += lax.dot_general(parts, gk, dims, preferred_element_type=jnp.float32)
        total += lax.dot_general(parts, fk, dims, preferred_element_type=jnp.float32)
        merged = gk.astype(jnp.float32) + fk.astype(jnp.float32)
        for j in range(CHUNK // LANES):
            m[k * (CHUNK // LANES) + j] = merged[:, j * LANES : (j + 1) * LANES]
    w[...] = jnp.zeros_like(w)
    w[:, :ROWS] = total[2 * RANK :] + total[RANK : 2 * RANK] + total[:RANK]
    left = w[...]
    for k in range(RANK):
        a_snd[k] = left[k : k + 1, :]
    a_rcv[me] = a_snd[me]
    strips[QUARTER] = jnp.zeros((ROWS, LANES), jnp.float32)

    pl.semaphore_wait(barrier, PLANE - 1 + 2 * REACH)
    for ahead in (REACH, DEEP - REACH):
        pl.semaphore_signal(reach, inc=1, device_id=deep(ahead)[0], device_id_type=MESH)

    spans = ((0, EARLY), (EARLY, QUARTER - EARLY))
    order = [(2, 0), (2, 1), (1, 1), (3, 0), (1, 0), (3, 1), (0, 0), (0, 1)]

    def pair_copy(step, core_to, place):
        ahead, span = order[step]
        start, size = spans[span]
        there = wrap(place + ahead, SIDE) * QUARTER + start
        src, dst = m.at[pl.ds(core_to * (STRIPS // 2) + there, size)], pr.at[pl.ds(there, size)]
        return remote(src, dst, d_s.at[step], d_r.at[step], partner)

    def paired(step):
        pair_copy(step, core, first).wait_recv()
        ahead, span = order[step]
        start, size = spans[span]
        there = wrap(first + ahead, SIDE) * QUARTER + start
        mine = m.at[pl.ds(core * (STRIPS // 2) + there, size)]
        mine[...] = mine[...] + pr[pl.ds(there, size)]
        return mine

    for step in range(8):
        pair_copy(step, 1 - core, then).start()

    for device, peer in plane:
        remote(a_snd.at[peer], a_rcv.at[me], row_sems.at[0], row_sems.at[1], device).start()

    above, below = at(wrap(first + 1, SIDE), then), at(wrap(first + 3, SIDE), then)
    upper, lower = pl.ds(EARLY, QUARTER - EARLY), pl.ds(0, EARLY)
    ring = []

    def pass_round(src, dst, device):
        index = len(ring)
        copy = remote(src, dst, p_s.at[index], p_r.at[index], device)
        copy.start()
        ring.append(copy)

    pass_round(paired(0), up_in, above)
    pass_round(paired(1), down_in, below)
    pass_round(paired(2), from_below.at[upper], above)
    pass_round(paired(3), from_above.at[lower], below)
    mine = paired(4)
    ring[0].wait_recv()
    mine[...] = mine[...] + up_in[...]
    pass_round(mine, from_below.at[lower], above)
    mine = paired(5)
    ring[1].wait_recv()
    mine[...] = mine[...] + down_in[...]
    pass_round(mine, from_above.at[upper], below)

    pl.semaphore_wait(reach, 2)
    arrived(row_sems.at[1], a_rcv.at[pl.ds(0, PLANE - 1)])
    own_row = jnp.sum(a_rcv[...], axis=0)
    s_snd[0] = own_row
    s_rcv[z] = own_row

    for device, _ in planes:
        remote(s_snd.at[0], s_rcv.at[z], row_sems.at[2], row_sems.at[3], device).start()

    paired(6)
    paired(7)
    for index in (2, 3, 4, 5):
        ring[index].wait_recv()
    base = core * (STRIPS // 2) + first * QUARTER
    for t in range(QUARTER):
        strips[t] = m[base + t] + (from_below[t] + from_above[t])

    def second_copy(ahead, slot):
        two = wrap(then + ahead, SIDE)
        src = strips.at[pl.ds(PAIR * two, PAIR)]
        return remote(src, second.at[slot], q_s.at[ahead - 1], q_r.at[ahead - 1], at(first, two))

    for ahead in (2, 1, 3):
        second_copy(ahead, ahead - 1).start()

    arrived(row_sems.at[3], s_rcv.at[pl.ds(0, DEEP - 1)])
    whole_row = jnp.sum(s_rcv[...], axis=0)
    t_snd[0] = whole_row
    t_rcv[me] = whole_row
    for device, _ in plane:
        remote(t_snd.at[0], t_rcv.at[me], row_sems.at[4], row_sems.at[5], device).start()

    for ahead in (1, 3, 2):
        second_copy(ahead, ahead - 1).wait_recv()
    for t in range(PAIR):
        strip = (strips[PAIR * then + t] + second[0, t]) + (second[1, t] + second[2, t])
        folded = fold(strip)
        for i in range(TILES):
            for p in range(8):
                zs[8 * t + p, i] = folded[8 * i + p : 8 * i + p + 1, :]
    zr[z] = zs[z]

    for device, peer in planes:
        remote(zs.at[peer], zr.at[z], piece_sems.at[0], piece_sems.at[1], device).start()

    arrived(row_sems.at[5], t_rcv.at[pl.ds(0, PLANE - 1)])
    tiles = [jnp.concatenate([t_rcv[8 * t + k] for k in range(8)], axis=0) for t in range(RANK // 8)]
    basis = jnp.concatenate(orthonormal(tiles), axis=0)
    scaled = basis * (1.0 / WORKERS)
    high = scaled.astype(jnp.bfloat16).astype(jnp.float32)
    split = jnp.concatenate([high, high, scaled - high, jnp.zeros((RANK, LANES), jnp.float32)], axis=0)
    lc[...] = jnp.transpose(split)[:ROWS].astype(jnp.bfloat16)

    arrived(piece_sems.at[1], zr.at[pl.ds(0, DEEP - 1)])
    piece = jnp.sum(zr[...], axis=0)
    row = lax.broadcasted_iota(jnp.int32, (8, LANES), 0)
    lane = lax.broadcasted_iota(jnp.int32, (8, LANES), 1)
    diagonal = (lane // PIECE) == row
    spread = [jnp.where(diagonal, jnp.broadcast_to(piece[i], (8, LANES)), 0.0) for i in range(TILES)]
    spread.append(jnp.zeros((LANES - ROWS, LANES), jnp.float32))
    part = jnp.dot(
        basis, jnp.concatenate(spread, axis=0), precision=lax.Precision.HIGHEST, preferred_element_type=jnp.float32
    )
    for step in (1, 2, 4):
        part = part + pltpu.roll(part, step * PIECE, 1)
    for k in range(RANK // 8):
        packed = jnp.where(diagonal, part[8 * k : 8 * k + 8], 0.0)
        pk[k] = jnp.sum(packed, axis=0, keepdims=True)
        zg[z, k] = pk[k]

    for device, _ in planes:
        remote(pk, zg.at[z], part_sems.at[0], part_sems.at[1], device).start()

    arrived(part_sems.at[1], zg.at[pl.ds(0, DEEP - 1)])

    def block_of(chip_at, of_core):
        one = jnp.where(of_core == 0, chip_at % SIDE, chip_at // SIDE)
        two = jnp.where(of_core == 0, chip_at // SIDE, chip_at % SIDE)
        return nb.at[of_core * SIDE + one, two]

    def spread_block(device, chip_at, slot):
        return remote(block_of(chip, core), block_of(slot, core), n_s.at[chip_at], n_r.at[slot], device)

    def pass_on(chip_at, of_core):
        block = block_of(chip_at, of_core)
        return remote(block, block, f_s.at[chip_at], f_r.at[chip_at], partner)

    for t in range(PAIR):
        rows = [zg[8 * t + p, k] for k in range(RANK // 8) for p in range(8)]
        nb[core * SIDE + first, then, :, t * LANES : (t + 1) * LANES] = fold(jnp.concatenate(rows, axis=0))
    for device, chip_at in chips:
        spread_block(device, chip_at, chip).start()
    pass_on(chip, core).start()

    width = QUARTER * LANES

    def finish(half, quarter):
        here = pl.ds(pl.multiple_of((half * SIDE + quarter) * width, LANES), width)
        new = jnp.concatenate([nb[half * SIDE + quarter, two] for two in range(SIDE)], axis=1)[:, :width]
        new_basis[:, here] = new
        high = new.astype(jnp.bfloat16)
        low = (new - high.astype(jnp.float32)).astype(jnp.bfloat16)
        parts = jnp.concatenate([high, low, high, jnp.zeros_like(high)], axis=0)
        approx = jnp.dot(lc[...], parts, preferred_element_type=jnp.float32)
        merged = g[:, here].astype(jnp.float32) + f[:, here].astype(jnp.float32)
        out[:, here] = (merged - approx).astype(jnp.bfloat16)

    for device, chip_at in reversed(chips):
        spread_block(device, chip_at, chip_at).wait_recv()
        pass_on(chip_at, core).start()

    @pl.loop(0, SIDE)
    def _(quarter):
        finish(core, quarter)

    @pl.loop(0, SIDE)
    def _(quarter):
        for two in range(SIDE):
            chip_at = jnp.where(core == 1, two * SIDE + quarter, quarter * SIDE + two)
            pass_on(chip_at, 1 - core).wait_recv()
        finish(1 - core, quarter)

    arrived(row_sems.at[0], a_rcv.at[pl.ds(0, PLANE - 1)])
    arrived(row_sems.at[2], s_rcv.at[pl.ds(0, DEEP - 1)])
    arrived(row_sems.at[4], t_rcv.at[pl.ds(0, PLANE - 1)])
    arrived(piece_sems.at[0], zr.at[pl.ds(0, DEEP - 1)])
    arrived(part_sems.at[0], zg.at[pl.ds(0, DEEP - 1)])
    for step in range(8):
        pair_copy(step, 1 - core, then).wait_send()
    for copy in ring:
        copy.wait_send()
    for ahead in (1, 2, 3):
        second_copy(ahead, ahead - 1).wait_send()
    for device, chip_at in chips:
        spread_block(device, chip_at, chip).wait_send()

    @pl.loop(0, CHIPS)
    def _(chip_at):
        pass_on(chip_at, core).wait_send()


def write(feedback, basis, feedback_out, basis_out, sems):
    copies = [
        pltpu.make_async_copy(feedback, feedback_out, sems.at[0]),
        pltpu.make_async_copy(basis, basis_out, sems.at[1]),
    ]
    for copy in copies:
        copy.start()
    for copy in copies:
        copy.wait()


def body(gradient, feedback, basis_in):
    f32, bf16 = jnp.float32, jnp.bfloat16
    dma = pltpu.SemaphoreType.DMA
    shapes = (jax.ShapeDtypeStruct((ROWS, FF), bf16), jax.ShapeDtypeStruct((RANK, FF), f32))
    new_feedback, new_basis = pl.pallas_call(
        kernel,
        out_shape=(pltpu.VMEM((ROWS, FF), bf16), pltpu.VMEM((RANK, FF), f32)),
        in_specs=[pl.BlockSpec(memory_space=pltpu.HBM)] * 3,
        out_specs=(pl.BlockSpec(memory_space=pltpu.VMEM),) * 2,
        scratch_shapes=[
            pltpu.VMEM((ROWS, FF), bf16),
            pltpu.VMEM((ROWS, FF), bf16),
            pltpu.VMEM((RANK, FF), f32),
            pltpu.VMEM((STRIPS, ROWS, LANES), f32),
            pltpu.VMEM((STRIPS // 2, ROWS, LANES), f32),
            pltpu.VMEM((EARLY, ROWS, LANES), f32),
            pltpu.VMEM((QUARTER - EARLY, ROWS, LANES), f32),
            pltpu.VMEM((QUARTER, ROWS, LANES), f32),
            pltpu.VMEM((QUARTER, ROWS, LANES), f32),
            pltpu.VMEM((SIDE * PAIR, ROWS, LANES), f32),
            pltpu.VMEM((SIDE - 1, PAIR, ROWS, LANES), f32),
            pltpu.VMEM((RANK, LANES), f32),
            pltpu.VMEM((PLANE, 1, LANES), f32),
            pltpu.VMEM((PLANE, 1, LANES), f32),
            pltpu.VMEM((1, 1, LANES), f32),
            pltpu.VMEM((DEEP, 1, LANES), f32),
            pltpu.VMEM((1, 1, LANES), f32),
            pltpu.VMEM((PLANE, 1, LANES), f32),
            pltpu.VMEM((DEEP, TILES, 1, LANES), f32),
            pltpu.VMEM((DEEP, TILES, 1, LANES), f32),
            pltpu.VMEM((RANK // 8, 1, LANES), f32),
            pltpu.VMEM((DEEP, RANK // 8, 1, LANES), f32),
            pltpu.VMEM((2 * SIDE, SIDE, RANK, PAIR * LANES), f32),
            pltpu.VMEM((ROWS, LANES), bf16),
            dma((LOADS, 3)),
            dma((6,)),
            dma((8,)), dma((8,)),
            dma((6,)), dma((6,)),
            dma((SIDE - 1,)), dma((SIDE - 1,)),
            dma((2,)),
            dma((2,)),
            dma((CHIPS,)), dma((CHIPS,)),
            dma((CHIPS,)), dma((CHIPS,)),
            pltpu.SemaphoreType.REGULAR,
        ],
        compiler_params=pltpu.CompilerParams(
            collective_id=0, has_side_effects=True, vmem_limit_bytes=65_093_632
        ),
        name="powersgd_step",
    )(gradient[0], feedback[0], basis_in.T)
    new_feedback, new_basis = pl.pallas_call(
        write,
        out_shape=shapes,
        in_specs=[pl.BlockSpec(memory_space=pl.ANY)] * 2,
        out_specs=(pl.BlockSpec(memory_space=pltpu.HBM),) * 2,
        scratch_shapes=[dma((2,))],
        compiler_params=pltpu.CompilerParams(vmem_limit_bytes=4 * 1024 * 1024),
        name="write_out",
    )(*(pltpu.with_memory_space_constraint(x, pltpu.VMEM) for x in (new_feedback, new_basis)))
    return new_feedback[None], new_basis.T


def solution(mesh):
    spec = P(("local", "dp"), None, None)
    return jax.shard_map(
        body, mesh=mesh, in_specs=(spec, spec, P()), out_specs=(spec, P()), check_vma=False
    )
```

```python
import jax
import jax.numpy as jnp
from jax import lax
from jax.experimental import pallas as pl
from jax.experimental.pallas import tpu as pltpu
from jax.sharding import PartitionSpec as P

MESH = pl.DeviceIdType.MESH

ROWS = 72
FF = 7168
RANK = 32
SIDE = 4
CHIPS = SIDE * SIDE
PLANE = 2 * CHIPS
DEEP = 16
REACH = DEEP // 4
LANES = 128
STRIPS = FF // LANES
QUARTER = STRIPS // 8
EARLY = 4
PAIR = 2
PIECE = PAIR * LANES // DEEP
TILES = ROWS // 8
LOADS = 7
CHUNK = FF // LOADS
WORKERS = 512
EPSILON = 1e-06


def wrap(value, size):
    return jnp.where(value >= size, value - size, value)


def fold(x):
    rows = x.shape[0]
    row = lax.broadcasted_iota(jnp.int32, x.shape, 0)
    lane = lax.broadcasted_iota(jnp.int32, x.shape, 1)
    for step in (1, 2, 4):
        low = (row & step) == 0
        near = (lane & (step * PIECE)) == 0
        up = pltpu.roll(pltpu.roll(x, rows - step, 0), step * PIECE, 1)
        down = pltpu.roll(pltpu.roll(x, step, 0), LANES - step * PIECE, 1)
        x = jnp.where(low & ~near, up, jnp.where(~low & near, down, x))
    return x


def orthonormal(tiles):
    row = lax.broadcasted_iota(jnp.int32, (8, LANES), 0)
    tiles = list(tiles)
    for index in range(RANK):
        own, at = divmod(index, 8)
        vector = jnp.broadcast_to(tiles[own][at : at + 1, :], (8, LANES))
        square = jnp.sum(vector * vector, axis=1, keepdims=True)
        inner = [jnp.sum(t * vector, axis=1, keepdims=True) for t in tiles[own:]]
        scale = lax.rsqrt(square + EPSILON)
        unit = vector * scale
        for later, product in enumerate(inner):
            moved = tiles[own + later] - (product * scale) * unit
            if later == 0:
                moved = jnp.where(row > at, moved, jnp.where(row == at, unit, tiles[own]))
            tiles[own + later] = moved
    return tiles


def kernel(
    g_hbm, f_hbm, b_hbm, out, new_basis,
    g, f, b, m, pr, up_in, down_in, from_below, from_above, strips, second,
    w, a_snd, a_rcv, s_snd, s_rcv, t_snd, t_rcv, zs, zr, pk, zg, nb, lc,
    ld, row_sems, d_s, d_r, p_s, p_r, q_s, q_r, piece_sems, part_sems, n_s, n_r, f_s, f_r, reach,
):
    y = lax.axis_index("local")
    dp = lax.axis_index("dp")
    z, x, core = dp // (2 * SIDE), (dp // 2) % SIDE, dp % 2
    chip = y * SIDE + x
    me = chip * 2 + core
    level = z * (2 * SIDE)
    partner = (y, level + 2 * x + 1 - core)
    first = jnp.where(core == 0, x, y)
    then = jnp.where(core == 0, y, x)

    def at(one, two):
        return (jnp.where(core == 0, two, one), level + 2 * jnp.where(core == 0, one, two) + core)

    def remote(src, dst, send, recv, device):
        return pltpu.make_async_remote_copy(
            src_ref=src, dst_ref=dst, send_sem=send, recv_sem=recv, device_id=device, device_id_type=MESH
        )

    def arrived(sem, ref):
        pltpu.make_async_copy(ref, ref, sem).wait()

    ys = [wrap(y + i, SIDE) for i in range(SIDE)]
    xs = [wrap(x + i, SIDE) for i in range(SIDE)]
    cores = [core, 1 - core]
    far = (0, 1, 2, 1)
    offsets = sorted(
        ((i, j, k) for i in range(SIDE) for j in range(SIDE) for k in range(2) if i + j + k),
        key=lambda o: -(far[o[0]] + far[o[1]]),
    )
    plane = [((ys[i], level + 2 * xs[j] + cores[k]), (ys[i] * SIDE + xs[j]) * 2 + cores[k]) for i, j, k in offsets]
    chips = [((ys[i], level + 2 * xs[j] + core), ys[i] * SIDE + xs[j]) for i, j, k in offsets if k == 0]

    def deep(i):
        peer = wrap(z + i, DEEP)
        return (y, peer * (2 * SIDE) + 2 * x + core), peer

    planes = [deep(i) for i in sorted(range(1, DEEP), key=lambda i: -min(i, DEEP - i))]

    def chunk(k):
        return pl.ds(k * CHUNK, CHUNK)

    loads = []
    for k in range(LOADS):
        some = []
        for index, (src, dst) in enumerate(((b_hbm, b), (g_hbm, g), (f_hbm, f))):
            copy = pltpu.make_async_copy(src.at[:, chunk(k)], dst.at[:, chunk(k)], ld.at[k, index])
            copy.start()
            some.append(copy)
        loads.append(some)

    barrier = pltpu.get_barrier_semaphore()
    for device, _ in plane:
        pl.semaphore_signal(barrier, inc=1, device_id=device, device_id_type=MESH)

    for i in range(1, REACH + 1):
        for ahead in (i, DEEP - i):
            pl.semaphore_signal(barrier, inc=1, device_id=deep(ahead)[0], device_id_type=MESH)

    total = jnp.zeros((3 * RANK, ROWS), jnp.float32)
    for k in range(LOADS):
        for copy in loads[k]:
            copy.wait()
        basis = b[:, k * CHUNK : (k + 1) * CHUNK]
        high = basis.astype(jnp.bfloat16)
        rest = basis - high.astype(jnp.float32)
        middle = rest.astype(jnp.bfloat16)
        low = (rest - middle.astype(jnp.float32)).astype(jnp.bfloat16)
        parts = jnp.concatenate([high, middle, low], axis=0)
        gk = g[:, k * CHUNK : (k + 1) * CHUNK]
        fk = f[:, k * CHUNK : (k + 1) * CHUNK]
        dims = (((1,), (1,)), ((), ()))
        total += lax.dot_general(parts, gk, dims, preferred_element_type=jnp.float32)
        total += lax.dot_general(parts, fk, dims, preferred_element_type=jnp.float32)
        merged = gk.astype(jnp.float32) + fk.astype(jnp.float32)
        for j in range(CHUNK // LANES):
            m[k * (CHUNK // LANES) + j] = merged[:, j * LANES : (j + 1) * LANES]
    w[...] = jnp.zeros_like(w)
    w[:, :ROWS] = total[2 * RANK :] + total[RANK : 2 * RANK] + total[:RANK]
    left = w[...]
    for k in range(RANK):
        a_snd[k] = left[k : k + 1, :]
    a_rcv[me] = a_snd[me]
    strips[QUARTER] = jnp.zeros((ROWS, LANES), jnp.float32)

    pl.semaphore_wait(barrier, PLANE - 1 + 2 * REACH)
    for ahead in (REACH, DEEP - REACH):
        pl.semaphore_signal(reach, inc=1, device_id=deep(ahead)[0], device_id_type=MESH)

    spans = ((0, EARLY), (EARLY, QUARTER - EARLY))
    order = [(2, 0), (2, 1), (1, 1), (3, 0), (1, 0), (3, 1), (0, 0), (0, 1)]

    def pair_copy(step, core_to, place):
        ahead, span = order[step]
        start, size = spans[span]
        there = wrap(place + ahead, SIDE) * QUARTER + start
        src, dst = m.at[pl.ds(core_to * (STRIPS // 2) + there, size)], pr.at[pl.ds(there, size)]
        return remote(src, dst, d_s.at[step], d_r.at[step], partner)

    def paired(step):
        pair_copy(step, core, first).wait_recv()
        ahead, span = order[step]
        start, size = spans[span]
        there = wrap(first + ahead, SIDE) * QUARTER + start
        mine = m.at[pl.ds(core * (STRIPS // 2) + there, size)]
        mine[...] = mine[...] + pr[pl.ds(there, size)]
        return mine

    for step in range(8):
        pair_copy(step, 1 - core, then).start()

    for device, peer in plane:
        remote(a_snd.at[peer], a_rcv.at[me], row_sems.at[0], row_sems.at[1], device).start()

    above, below = at(wrap(first + 1, SIDE), then), at(wrap(first + 3, SIDE), then)
    upper, lower = pl.ds(EARLY, QUARTER - EARLY), pl.ds(0, EARLY)
    ring = []

    def pass_round(src, dst, device):
        index = len(ring)
        copy = remote(src, dst, p_s.at[index], p_r.at[index], device)
        copy.start()
        ring.append(copy)

    pass_round(paired(0), up_in, above)
    pass_round(paired(1), down_in, below)
    pass_round(paired(2), from_below.at[upper], above)
    pass_round(paired(3), from_above.at[lower], below)
    mine = paired(4)
    ring[0].wait_recv()
    mine[...] = mine[...] + up_in[...]
    pass_round(mine, from_below.at[lower], above)
    mine = paired(5)
    ring[1].wait_recv()
    mine[...] = mine[...] + down_in[...]
    pass_round(mine, from_above.at[upper], below)

    pl.semaphore_wait(reach, 2)
    arrived(row_sems.at[1], a_rcv.at[pl.ds(0, PLANE - 1)])
    own_row = jnp.sum(a_rcv[...], axis=0)
    s_snd[0] = own_row
    s_rcv[z] = own_row

    for device, _ in planes:
        remote(s_snd.at[0], s_rcv.at[z], row_sems.at[2], row_sems.at[3], device).start()

    paired(6)
    paired(7)
    for index in (2, 3, 4, 5):
        ring[index].wait_recv()
    base = core * (STRIPS // 2) + first * QUARTER
    for t in range(QUARTER):
        strips[t] = m[base + t] + (from_below[t] + from_above[t])

    def second_copy(ahead, slot):
        two = wrap(then + ahead, SIDE)
        src = strips.at[pl.ds(PAIR * two, PAIR)]
        return remote(src, second.at[slot], q_s.at[ahead - 1], q_r.at[ahead - 1], at(first, two))

    for ahead in (2, 1, 3):
        second_copy(ahead, ahead - 1).start()

    arrived(row_sems.at[3], s_rcv.at[pl.ds(0, DEEP - 1)])
    whole_row = jnp.sum(s_rcv[...], axis=0)
    t_snd[0] = whole_row
    t_rcv[me] = whole_row
    for device, _ in plane:
        remote(t_snd.at[0], t_rcv.at[me], row_sems.at[4], row_sems.at[5], device).start()

    for ahead in (1, 3, 2):
        second_copy(ahead, ahead - 1).wait_recv()
    for t in range(PAIR):
        strip = (strips[PAIR * then + t] + second[0, t]) + (second[1, t] + second[2, t])
        folded = fold(strip)
        for i in range(TILES):
            for p in range(8):
                zs[8 * t + p, i] = folded[8 * i + p : 8 * i + p + 1, :]
    zr[z] = zs[z]

    for device, peer in planes:
        remote(zs.at[peer], zr.at[z], piece_sems.at[0], piece_sems.at[1], device).start()

    arrived(row_sems.at[5], t_rcv.at[pl.ds(0, PLANE - 1)])
    tiles = [jnp.concatenate([t_rcv[8 * t + k] for k in range(8)], axis=0) for t in range(RANK // 8)]
    basis = jnp.concatenate(orthonormal(tiles), axis=0)
    scaled = basis * (1.0 / WORKERS)
    high = scaled.astype(jnp.bfloat16).astype(jnp.float32)
    split = jnp.concatenate([high, high, scaled - high, jnp.zeros((RANK, LANES), jnp.float32)], axis=0)
    lc[...] = jnp.transpose(split)[:ROWS].astype(jnp.bfloat16)

    arrived(piece_sems.at[1], zr.at[pl.ds(0, DEEP - 1)])
    piece = jnp.sum(zr[...], axis=0)
    row = lax.broadcasted_iota(jnp.int32, (8, LANES), 0)
    lane = lax.broadcasted_iota(jnp.int32, (8, LANES), 1)
    diagonal = (lane // PIECE) == row
    spread = [jnp.where(diagonal, jnp.broadcast_to(piece[i], (8, LANES)), 0.0) for i in range(TILES)]
    spread.append(jnp.zeros((LANES - ROWS, LANES), jnp.float32))
    part = jnp.dot(
        basis, jnp.concatenate(spread, axis=0), precision=lax.Precision.HIGHEST, preferred_element_type=jnp.float32
    )
    for step in (1, 2, 4):
        part = part + pltpu.roll(part, step * PIECE, 1)
    for k in range(RANK // 8):
        packed = jnp.where(diagonal, part[8 * k : 8 * k + 8], 0.0)
        pk[k] = jnp.sum(packed, axis=0, keepdims=True)
        zg[z, k] = pk[k]

    for device, _ in planes:
        remote(pk, zg.at[z], part_sems.at[0], part_sems.at[1], device).start()

    arrived(part_sems.at[1], zg.at[pl.ds(0, DEEP - 1)])

    def block_of(chip_at, of_core):
        one = jnp.where(of_core == 0, chip_at % SIDE, chip_at // SIDE)
        two = jnp.where(of_core == 0, chip_at // SIDE, chip_at % SIDE)
        return nb.at[of_core * SIDE + one, two]

    def spread_block(device, chip_at, slot):
        return remote(block_of(chip, core), block_of(slot, core), n_s.at[chip_at], n_r.at[slot], device)

    def pass_on(chip_at, of_core):
        block = block_of(chip_at, of_core)
        return remote(block, block, f_s.at[chip_at], f_r.at[chip_at], partner)

    for t in range(PAIR):
        rows = [zg[8 * t + p, k] for k in range(RANK // 8) for p in range(8)]
        nb[core * SIDE + first, then, :, t * LANES : (t + 1) * LANES] = fold(jnp.concatenate(rows, axis=0))
    for device, chip_at in chips:
        spread_block(device, chip_at, chip).start()
    pass_on(chip, core).start()

    width = QUARTER * LANES

    def finish(half, quarter):
        here = pl.ds(pl.multiple_of((half * SIDE + quarter) * width, LANES), width)
        new = jnp.concatenate([nb[half * SIDE + quarter, two] for two in range(SIDE)], axis=1)[:, :width]
        new_basis[:, here] = new
        high = new.astype(jnp.bfloat16)
        low = (new - high.astype(jnp.float32)).astype(jnp.bfloat16)
        parts = jnp.concatenate([high, low, high, jnp.zeros_like(high)], axis=0)
        approx = jnp.dot(lc[...], parts, preferred_element_type=jnp.float32)
        merged = g[:, here].astype(jnp.float32) + f[:, here].astype(jnp.float32)
        out[:, here] = (merged - approx).astype(jnp.bfloat16)

    for device, chip_at in chips:
        spread_block(device, chip_at, chip_at).wait_recv()
        pass_on(chip_at, core).start()

    @pl.loop(0, SIDE)
    def _(quarter):
        finish(core, quarter)

    @pl.loop(0, SIDE)
    def _(quarter):
        for two in range(SIDE):
            chip_at = jnp.where(core == 1, two * SIDE + quarter, quarter * SIDE + two)
            pass_on(chip_at, 1 - core).wait_recv()
        finish(1 - core, quarter)

    arrived(row_sems.at[0], a_rcv.at[pl.ds(0, PLANE - 1)])
    arrived(row_sems.at[2], s_rcv.at[pl.ds(0, DEEP - 1)])
    arrived(row_sems.at[4], t_rcv.at[pl.ds(0, PLANE - 1)])
    arrived(piece_sems.at[0], zr.at[pl.ds(0, DEEP - 1)])
    arrived(part_sems.at[0], zg.at[pl.ds(0, DEEP - 1)])
    for step in range(8):
        pair_copy(step, 1 - core, then).wait_send()
    for copy in ring:
        copy.wait_send()
    for ahead in (1, 2, 3):
        second_copy(ahead, ahead - 1).wait_send()
    for device, chip_at in chips:
        spread_block(device, chip_at, chip).wait_send()

    @pl.loop(0, CHIPS)
    def _(chip_at):
        pass_on(chip_at, core).wait_send()


def write(feedback, basis, feedback_out, basis_out, sems):
    copies = [
        pltpu.make_async_copy(feedback, feedback_out, sems.at[0]),
        pltpu.make_async_copy(basis, basis_out, sems.at[1]),
    ]
    for copy in copies:
        copy.start()
    for copy in copies:
        copy.wait()


def body(gradient, feedback, basis_in):
    f32, bf16 = jnp.float32, jnp.bfloat16
    dma = pltpu.SemaphoreType.DMA
    shapes = (jax.ShapeDtypeStruct((ROWS, FF), bf16), jax.ShapeDtypeStruct((RANK, FF), f32))
    new_feedback, new_basis = pl.pallas_call(
        kernel,
        out_shape=(pltpu.VMEM((ROWS, FF), bf16), pltpu.VMEM((RANK, FF), f32)),
        in_specs=[pl.BlockSpec(memory_space=pltpu.HBM)] * 3,
        out_specs=(pl.BlockSpec(memory_space=pltpu.VMEM),) * 2,
        scratch_shapes=[
            pltpu.VMEM((ROWS, FF), bf16),
            pltpu.VMEM((ROWS, FF), bf16),
            pltpu.VMEM((RANK, FF), f32),
            pltpu.VMEM((STRIPS, ROWS, LANES), f32),
            pltpu.VMEM((STRIPS // 2, ROWS, LANES), f32),
            pltpu.VMEM((EARLY, ROWS, LANES), f32),
            pltpu.VMEM((QUARTER - EARLY, ROWS, LANES), f32),
            pltpu.VMEM((QUARTER, ROWS, LANES), f32),
            pltpu.VMEM((QUARTER, ROWS, LANES), f32),
            pltpu.VMEM((SIDE * PAIR, ROWS, LANES), f32),
            pltpu.VMEM((SIDE - 1, PAIR, ROWS, LANES), f32),
            pltpu.VMEM((RANK, LANES), f32),
            pltpu.VMEM((PLANE, 1, LANES), f32),
            pltpu.VMEM((PLANE, 1, LANES), f32),
            pltpu.VMEM((1, 1, LANES), f32),
            pltpu.VMEM((DEEP, 1, LANES), f32),
            pltpu.VMEM((1, 1, LANES), f32),
            pltpu.VMEM((PLANE, 1, LANES), f32),
            pltpu.VMEM((DEEP, TILES, 1, LANES), f32),
            pltpu.VMEM((DEEP, TILES, 1, LANES), f32),
            pltpu.VMEM((RANK // 8, 1, LANES), f32),
            pltpu.VMEM((DEEP, RANK // 8, 1, LANES), f32),
            pltpu.VMEM((2 * SIDE, SIDE, RANK, PAIR * LANES), f32),
            pltpu.VMEM((ROWS, LANES), bf16),
            dma((LOADS, 3)),
            dma((6,)),
            dma((8,)), dma((8,)),
            dma((6,)), dma((6,)),
            dma((SIDE - 1,)), dma((SIDE - 1,)),
            dma((2,)),
            dma((2,)),
            dma((CHIPS,)), dma((CHIPS,)),
            dma((CHIPS,)), dma((CHIPS,)),
            pltpu.SemaphoreType.REGULAR,
        ],
        compiler_params=pltpu.CompilerParams(
            collective_id=0, has_side_effects=True, vmem_limit_bytes=65_093_632
        ),
        name="powersgd_step",
    )(gradient[0], feedback[0], basis_in.T)
    new_feedback, new_basis = pl.pallas_call(
        write,
        out_shape=shapes,
        in_specs=[pl.BlockSpec(memory_space=pl.ANY)] * 2,
        out_specs=(pl.BlockSpec(memory_space=pltpu.HBM),) * 2,
        scratch_shapes=[dma((2,))],
        compiler_params=pltpu.CompilerParams(vmem_limit_bytes=4 * 1024 * 1024),
        name="write_out",
    )(*(pltpu.with_memory_space_constraint(x, pltpu.VMEM) for x in (new_feedback, new_basis)))
    return new_feedback[None], new_basis.T


def solution(mesh):
    spec = P(("local", "dp"), None, None)
    return jax.shard_map(
        body, mesh=mesh, in_specs=(spec, spec, P()), out_specs=(spec, P()), check_vma=False
    )
```

```python
import jax
import jax.numpy as jnp
from jax import lax
from jax.experimental import pallas as pl
from jax.experimental.pallas import tpu as pltpu
from jax.sharding import PartitionSpec as P

MESH = pl.DeviceIdType.MESH

ROWS = 72
FF = 7168
RANK = 32
SIDE = 4
CHIPS = SIDE * SIDE
PLANE = 2 * CHIPS
DEEP = 16
REACH = DEEP // 4
LANES = 128
STRIPS = FF // LANES
QUARTER = STRIPS // 8
EARLY = 4
PAIR = 2
PIECE = PAIR * LANES // DEEP
TILES = ROWS // 8
LOADS = 14
CHUNK = FF // LOADS
WORKERS = 512
EPSILON = 1e-06


def wrap(value, size):
    return jnp.where(value >= size, value - size, value)


def fold(x):
    rows = x.shape[0]
    row = lax.broadcasted_iota(jnp.int32, x.shape, 0)
    lane = lax.broadcasted_iota(jnp.int32, x.shape, 1)
    for step in (1, 2, 4):
        low = (row & step) == 0
        near = (lane & (step * PIECE)) == 0
        up = pltpu.roll(pltpu.roll(x, rows - step, 0), step * PIECE, 1)
        down = pltpu.roll(pltpu.roll(x, step, 0), LANES - step * PIECE, 1)
        x = jnp.where(low & ~near, up, jnp.where(~low & near, down, x))
    return x


def orthonormal(tiles):
    row = lax.broadcasted_iota(jnp.int32, (8, LANES), 0)
    tiles = list(tiles)
    for index in range(RANK):
        own, at = divmod(index, 8)
        vector = jnp.broadcast_to(tiles[own][at : at + 1, :], (8, LANES))
        square = jnp.sum(vector * vector, axis=1, keepdims=True)
        inner = [jnp.sum(t * vector, axis=1, keepdims=True) for t in tiles[own:]]
        scale = lax.rsqrt(square + EPSILON)
        unit = vector * scale
        for later, product in enumerate(inner):
            moved = tiles[own + later] - (product * scale) * unit
            if later == 0:
                moved = jnp.where(row > at, moved, jnp.where(row == at, unit, tiles[own]))
            tiles[own + later] = moved
    return tiles


def kernel(
    g_hbm, f_hbm, b_hbm, out, new_basis,
    g, f, b, m, pr, up_in, down_in, from_below, from_above, strips, second,
    w, a_snd, a_rcv, s_snd, s_rcv, t_snd, t_rcv, zs, zr, pk, zg, nb, lc,
    ld, row_sems, d_s, d_r, p_s, p_r, q_s, q_r, piece_sems, part_sems, n_s, n_r, f_s, f_r, reach,
):
    y = lax.axis_index("local")
    dp = lax.axis_index("dp")
    z, x, core = dp // (2 * SIDE), (dp // 2) % SIDE, dp % 2
    chip = y * SIDE + x
    me = chip * 2 + core
    level = z * (2 * SIDE)
    partner = (y, level + 2 * x + 1 - core)
    first = jnp.where(core == 0, x, y)
    then = jnp.where(core == 0, y, x)

    def at(one, two):
        return (jnp.where(core == 0, two, one), level + 2 * jnp.where(core == 0, one, two) + core)

    def remote(src, dst, send, recv, device):
        return pltpu.make_async_remote_copy(
            src_ref=src, dst_ref=dst, send_sem=send, recv_sem=recv, device_id=device, device_id_type=MESH
        )

    def arrived(sem, ref):
        pltpu.make_async_copy(ref, ref, sem).wait()

    ys = [wrap(y + i, SIDE) for i in range(SIDE)]
    xs = [wrap(x + i, SIDE) for i in range(SIDE)]
    cores = [core, 1 - core]
    far = (0, 1, 2, 1)
    offsets = sorted(
        ((i, j, k) for i in range(SIDE) for j in range(SIDE) for k in range(2) if i + j + k),
        key=lambda o: -(far[o[0]] + far[o[1]]),
    )
    plane = [((ys[i], level + 2 * xs[j] + cores[k]), (ys[i] * SIDE + xs[j]) * 2 + cores[k]) for i, j, k in offsets]
    chips = [((ys[i], level + 2 * xs[j] + core), ys[i] * SIDE + xs[j]) for i, j, k in offsets if k == 0]

    def deep(i):
        peer = wrap(z + i, DEEP)
        return (y, peer * (2 * SIDE) + 2 * x + core), peer

    planes = [deep(i) for i in sorted(range(1, DEEP), key=lambda i: -min(i, DEEP - i))]

    def chunk(k):
        return pl.ds(k * CHUNK, CHUNK)

    loads = []
    for k in range(LOADS):
        some = []
        for index, (src, dst) in enumerate(((b_hbm, b), (g_hbm, g), (f_hbm, f))):
            copy = pltpu.make_async_copy(src.at[:, chunk(k)], dst.at[:, chunk(k)], ld.at[k, index])
            copy.start()
            some.append(copy)
        loads.append(some)

    barrier = pltpu.get_barrier_semaphore()
    for device, _ in plane:
        pl.semaphore_signal(barrier, inc=1, device_id=device, device_id_type=MESH)

    for i in range(1, REACH + 1):
        for ahead in (i, DEEP - i):
            pl.semaphore_signal(barrier, inc=1, device_id=deep(ahead)[0], device_id_type=MESH)

    total = jnp.zeros((3 * RANK, ROWS), jnp.float32)
    for k in range(LOADS):
        for copy in loads[k]:
            copy.wait()
        basis = b[:, k * CHUNK : (k + 1) * CHUNK]
        high = basis.astype(jnp.bfloat16)
        rest = basis - high.astype(jnp.float32)
        middle = rest.astype(jnp.bfloat16)
        low = (rest - middle.astype(jnp.float32)).astype(jnp.bfloat16)
        parts = jnp.concatenate([high, middle, low], axis=0)
        gk = g[:, k * CHUNK : (k + 1) * CHUNK]
        fk = f[:, k * CHUNK : (k + 1) * CHUNK]
        dims = (((1,), (1,)), ((), ()))
        total += lax.dot_general(parts, gk, dims, preferred_element_type=jnp.float32)
        total += lax.dot_general(parts, fk, dims, preferred_element_type=jnp.float32)
        merged = gk.astype(jnp.float32) + fk.astype(jnp.float32)
        for j in range(CHUNK // LANES):
            m[k * (CHUNK // LANES) + j] = merged[:, j * LANES : (j + 1) * LANES]
    w[...] = jnp.zeros_like(w)
    w[:, :ROWS] = total[2 * RANK :] + total[RANK : 2 * RANK] + total[:RANK]
    left = w[...]
    for k in range(RANK):
        a_snd[k] = left[k : k + 1, :]
    a_rcv[me] = a_snd[me]
    strips[QUARTER] = jnp.zeros((ROWS, LANES), jnp.float32)

    pl.semaphore_wait(barrier, PLANE - 1 + 2 * REACH)
    for ahead in (REACH, DEEP - REACH):
        pl.semaphore_signal(reach, inc=1, device_id=deep(ahead)[0], device_id_type=MESH)

    spans = ((0, EARLY), (EARLY, QUARTER - EARLY))
    order = [(2, 0), (2, 1), (1, 1), (3, 0), (1, 0), (3, 1), (0, 0), (0, 1)]

    def pair_copy(step, core_to, place):
        ahead, span = order[step]
        start, size = spans[span]
        there = wrap(place + ahead, SIDE) * QUARTER + start
        src, dst = m.at[pl.ds(core_to * (STRIPS // 2) + there, size)], pr.at[pl.ds(there, size)]
        return remote(src, dst, d_s.at[step], d_r.at[step], partner)

    def paired(step):
        pair_copy(step, core, first).wait_recv()
        ahead, span = order[step]
        start, size = spans[span]
        there = wrap(first + ahead, SIDE) * QUARTER + start
        mine = m.at[pl.ds(core * (STRIPS // 2) + there, size)]
        mine[...] = mine[...] + pr[pl.ds(there, size)]
        return mine

    for step in range(8):
        pair_copy(step, 1 - core, then).start()

    for device, peer in plane:
        remote(a_snd.at[peer], a_rcv.at[me], row_sems.at[0], row_sems.at[1], device).start()

    above, below = at(wrap(first + 1, SIDE), then), at(wrap(first + 3, SIDE), then)
    upper, lower = pl.ds(EARLY, QUARTER - EARLY), pl.ds(0, EARLY)
    ring = []

    def pass_round(src, dst, device):
        index = len(ring)
        copy = remote(src, dst, p_s.at[index], p_r.at[index], device)
        copy.start()
        ring.append(copy)

    pass_round(paired(0), up_in, above)
    pass_round(paired(1), down_in, below)
    pass_round(paired(2), from_below.at[upper], above)
    pass_round(paired(3), from_above.at[lower], below)
    mine = paired(4)
    ring[0].wait_recv()
    mine[...] = mine[...] + up_in[...]
    pass_round(mine, from_below.at[lower], above)
    mine = paired(5)
    ring[1].wait_recv()
    mine[...] = mine[...] + down_in[...]
    pass_round(mine, from_above.at[upper], below)

    pl.semaphore_wait(reach, 2)
    arrived(row_sems.at[1], a_rcv.at[pl.ds(0, PLANE - 1)])
    own_row = jnp.sum(a_rcv[...], axis=0)
    s_snd[0] = own_row
    s_rcv[z] = own_row

    for device, _ in planes:
        remote(s_snd.at[0], s_rcv.at[z], row_sems.at[2], row_sems.at[3], device).start()

    paired(6)
    paired(7)
    for index in (2, 3, 4, 5):
        ring[index].wait_recv()
    base = core * (STRIPS // 2) + first * QUARTER
    for t in range(QUARTER):
        strips[t] = m[base + t] + (from_below[t] + from_above[t])

    def second_copy(ahead, slot):
        two = wrap(then + ahead, SIDE)
        src = strips.at[pl.ds(PAIR * two, PAIR)]
        return remote(src, second.at[slot], q_s.at[ahead - 1], q_r.at[ahead - 1], at(first, two))

    for ahead in (2, 1, 3):
        second_copy(ahead, ahead - 1).start()

    arrived(row_sems.at[3], s_rcv.at[pl.ds(0, DEEP - 1)])
    whole_row = jnp.sum(s_rcv[...], axis=0)
    t_snd[0] = whole_row
    t_rcv[me] = whole_row
    for device, _ in plane:
        remote(t_snd.at[0], t_rcv.at[me], row_sems.at[4], row_sems.at[5], device).start()

    for ahead in (1, 3, 2):
        second_copy(ahead, ahead - 1).wait_recv()
    for t in range(PAIR):
        strip = (strips[PAIR * then + t] + second[0, t]) + (second[1, t] + second[2, t])
        folded = fold(strip)
        for i in range(TILES):
            for p in range(8):
                zs[8 * t + p, i] = folded[8 * i + p : 8 * i + p + 1, :]
    zr[z] = zs[z]

    for device, peer in planes:
        remote(zs.at[peer], zr.at[z], piece_sems.at[0], piece_sems.at[1], device).start()

    arrived(row_sems.at[5], t_rcv.at[pl.ds(0, PLANE - 1)])
    tiles = [jnp.concatenate([t_rcv[8 * t + k] for k in range(8)], axis=0) for t in range(RANK // 8)]
    basis = jnp.concatenate(orthonormal(tiles), axis=0)
    scaled = basis * (1.0 / WORKERS)
    high = scaled.astype(jnp.bfloat16).astype(jnp.float32)
    split = jnp.concatenate([high, high, scaled - high, jnp.zeros((RANK, LANES), jnp.float32)], axis=0)
    lc[...] = jnp.transpose(split)[:ROWS].astype(jnp.bfloat16)

    arrived(piece_sems.at[1], zr.at[pl.ds(0, DEEP - 1)])
    piece = jnp.sum(zr[...], axis=0)
    row = lax.broadcasted_iota(jnp.int32, (8, LANES), 0)
    lane = lax.broadcasted_iota(jnp.int32, (8, LANES), 1)
    diagonal = (lane // PIECE) == row
    spread = [jnp.where(diagonal, jnp.broadcast_to(piece[i], (8, LANES)), 0.0) for i in range(TILES)]
    spread.append(jnp.zeros((LANES - ROWS, LANES), jnp.float32))
    part = jnp.dot(
        basis, jnp.concatenate(spread, axis=0), precision=lax.Precision.HIGHEST, preferred_element_type=jnp.float32
    )
    for step in (1, 2, 4):
        part = part + pltpu.roll(part, step * PIECE, 1)
    for k in range(RANK // 8):
        packed = jnp.where(diagonal, part[8 * k : 8 * k + 8], 0.0)
        pk[k] = jnp.sum(packed, axis=0, keepdims=True)
        zg[z, k] = pk[k]

    for device, _ in planes:
        remote(pk, zg.at[z], part_sems.at[0], part_sems.at[1], device).start()

    arrived(part_sems.at[1], zg.at[pl.ds(0, DEEP - 1)])

    def block_of(chip_at, of_core):
        one = jnp.where(of_core == 0, chip_at % SIDE, chip_at // SIDE)
        two = jnp.where(of_core == 0, chip_at // SIDE, chip_at % SIDE)
        return nb.at[of_core * SIDE + one, two]

    def spread_block(device, chip_at, slot):
        return remote(block_of(chip, core), block_of(slot, core), n_s.at[chip_at], n_r.at[slot], device)

    def pass_on(chip_at, of_core):
        block = block_of(chip_at, of_core)
        return remote(block, block, f_s.at[chip_at], f_r.at[chip_at], partner)

    for t in range(PAIR):
        rows = [zg[8 * t + p, k] for k in range(RANK // 8) for p in range(8)]
        nb[core * SIDE + first, then, :, t * LANES : (t + 1) * LANES] = fold(jnp.concatenate(rows, axis=0))
    for device, chip_at in chips:
        spread_block(device, chip_at, chip).start()
    pass_on(chip, core).start()

    width = QUARTER * LANES

    def finish(half, quarter):
        here = pl.ds(pl.multiple_of((half * SIDE + quarter) * width, LANES), width)
        new = jnp.concatenate([nb[half * SIDE + quarter, two] for two in range(SIDE)], axis=1)[:, :width]
        new_basis[:, here] = new
        high = new.astype(jnp.bfloat16)
        low = (new - high.astype(jnp.float32)).astype(jnp.bfloat16)
        parts = jnp.concatenate([high, low, high, jnp.zeros_like(high)], axis=0)
        approx = jnp.dot(lc[...], parts, preferred_element_type=jnp.float32)
        merged = g[:, here].astype(jnp.float32) + f[:, here].astype(jnp.float32)
        out[:, here] = (merged - approx).astype(jnp.bfloat16)

    for device, chip_at in reversed(chips):
        spread_block(device, chip_at, chip_at).wait_recv()
        pass_on(chip_at, core).start()

    @pl.loop(0, SIDE)
    def _(quarter):
        finish(core, quarter)

    @pl.loop(0, SIDE)
    def _(quarter):
        for two in range(SIDE):
            chip_at = jnp.where(core == 1, two * SIDE + quarter, quarter * SIDE + two)
            pass_on(chip_at, 1 - core).wait_recv()
        finish(1 - core, quarter)

    arrived(row_sems.at[0], a_rcv.at[pl.ds(0, PLANE - 1)])
    arrived(row_sems.at[2], s_rcv.at[pl.ds(0, DEEP - 1)])
    arrived(row_sems.at[4], t_rcv.at[pl.ds(0, PLANE - 1)])
    arrived(piece_sems.at[0], zr.at[pl.ds(0, DEEP - 1)])
    arrived(part_sems.at[0], zg.at[pl.ds(0, DEEP - 1)])
    for step in range(8):
        pair_copy(step, 1 - core, then).wait_send()
    for copy in ring:
        copy.wait_send()
    for ahead in (1, 2, 3):
        second_copy(ahead, ahead - 1).wait_send()
    for device, chip_at in chips:
        spread_block(device, chip_at, chip).wait_send()

    @pl.loop(0, CHIPS)
    def _(chip_at):
        pass_on(chip_at, core).wait_send()


def write(feedback, basis, feedback_out, basis_out, sems):
    copies = [
        pltpu.make_async_copy(feedback, feedback_out, sems.at[0]),
        pltpu.make_async_copy(basis, basis_out, sems.at[1]),
    ]
    for copy in copies:
        copy.start()
    for copy in copies:
        copy.wait()


def body(gradient, feedback, basis_in):
    f32, bf16 = jnp.float32, jnp.bfloat16
    dma = pltpu.SemaphoreType.DMA
    shapes = (jax.ShapeDtypeStruct((ROWS, FF), bf16), jax.ShapeDtypeStruct((RANK, FF), f32))
    new_feedback, new_basis = pl.pallas_call(
        kernel,
        out_shape=(pltpu.VMEM((ROWS, FF), bf16), pltpu.VMEM((RANK, FF), f32)),
        in_specs=[pl.BlockSpec(memory_space=pltpu.HBM)] * 3,
        out_specs=(pl.BlockSpec(memory_space=pltpu.VMEM),) * 2,
        scratch_shapes=[
            pltpu.VMEM((ROWS, FF), bf16),
            pltpu.VMEM((ROWS, FF), bf16),
            pltpu.VMEM((RANK, FF), f32),
            pltpu.VMEM((STRIPS, ROWS, LANES), f32),
            pltpu.VMEM((STRIPS // 2, ROWS, LANES), f32),
            pltpu.VMEM((EARLY, ROWS, LANES), f32),
            pltpu.VMEM((QUARTER - EARLY, ROWS, LANES), f32),
            pltpu.VMEM((QUARTER, ROWS, LANES), f32),
            pltpu.VMEM((QUARTER, ROWS, LANES), f32),
            pltpu.VMEM((SIDE * PAIR, ROWS, LANES), f32),
            pltpu.VMEM((SIDE - 1, PAIR, ROWS, LANES), f32),
            pltpu.VMEM((RANK, LANES), f32),
            pltpu.VMEM((PLANE, 1, LANES), f32),
            pltpu.VMEM((PLANE, 1, LANES), f32),
            pltpu.VMEM((1, 1, LANES), f32),
            pltpu.VMEM((DEEP, 1, LANES), f32),
            pltpu.VMEM((1, 1, LANES), f32),
            pltpu.VMEM((PLANE, 1, LANES), f32),
            pltpu.VMEM((DEEP, TILES, 1, LANES), f32),
            pltpu.VMEM((DEEP, TILES, 1, LANES), f32),
            pltpu.VMEM((RANK // 8, 1, LANES), f32),
            pltpu.VMEM((DEEP, RANK // 8, 1, LANES), f32),
            pltpu.VMEM((2 * SIDE, SIDE, RANK, PAIR * LANES), f32),
            pltpu.VMEM((ROWS, LANES), bf16),
            dma((LOADS, 3)),
            dma((6,)),
            dma((8,)), dma((8,)),
            dma((6,)), dma((6,)),
            dma((SIDE - 1,)), dma((SIDE - 1,)),
            dma((2,)),
            dma((2,)),
            dma((CHIPS,)), dma((CHIPS,)),
            dma((CHIPS,)), dma((CHIPS,)),
            pltpu.SemaphoreType.REGULAR,
        ],
        compiler_params=pltpu.CompilerParams(
            collective_id=0, has_side_effects=True, vmem_limit_bytes=65_093_632
        ),
        name="powersgd_step",
    )(gradient[0], feedback[0], basis_in.T)
    new_feedback, new_basis = pl.pallas_call(
        write,
        out_shape=shapes,
        in_specs=[pl.BlockSpec(memory_space=pl.ANY)] * 2,
        out_specs=(pl.BlockSpec(memory_space=pltpu.HBM),) * 2,
        scratch_shapes=[dma((2,))],
        compiler_params=pltpu.CompilerParams(vmem_limit_bytes=4 * 1024 * 1024),
        name="write_out",
    )(*(pltpu.with_memory_space_constraint(x, pltpu.VMEM) for x in (new_feedback, new_basis)))
    return new_feedback[None], new_basis.T


def solution(mesh):
    spec = P(("local", "dp"), None, None)
    return jax.shard_map(
        body, mesh=mesh, in_specs=(spec, spec, P()), out_specs=(spec, P()), check_vma=False
    )
```
